256 devices in a mesh: seq: 32 (over y, x, core), grp: 8 (over z).
Axes of the slice: x: 4, y: 4, z: 8, core: 2. Of those that a mesh axis runs over, the one named last changes fastest.
Arguments:
- queries: bfloat16 [32768, 8, 128], P(('grp', 'seq')), may hold values from -6 to 6
- key_rows: bfloat16 [32768, 8, 128], P(('grp', 'seq')), may hold values from -6 to 6
- value_rows: bfloat16 [32768, 8, 256], P(('grp', 'seq')), may hold values from -6 to 6
- log_gate: float32 [8, 32768], P(None, ('grp', 'seq')), may hold values from -1.5 to 0
- beta_rate: float32 [8, 32768], P(None, ('grp', 'seq')), may hold values from 0 to 0.9
Outputs:
- outputs: bfloat16 [32768, 8, 256], P(('grp', 'seq'))
The draws below stay inside these ranges and needn't reach their ends.
All inputs are finite; a program needn't handle non-finite values.
Results may differ from the reference program's by a relative error of at most 0.0012.
Values sent between devices are 32-bit elements; how exact they have to be, the bound alone decides.
A program may use at most 128 MiB of HBM per device.

```python
import math
import jax
import jax.numpy as jnp
from jax import lax

H = 8
K = 128
V = 256
STRETCH = 64
TOK_DEV = 128
TOKENS = 32768


def gate_parts(key):
    order_ids = jax.random.permutation(jax.random.fold_in(key, 101), H)
    quick_heads = order_ids < H // 2
    block_count = TOKENS // TOK_DEV
    spread = jax.random.uniform(jax.random.fold_in(key, 102), (H, block_count), jnp.float32, -0.7, 0.7)
    device_factor = jnp.repeat(jnp.exp(spread), TOK_DEV, axis=1)
    fast_base = max(1.0 / 40.0, 4.0 / TOK_DEV) * jnp.exp(jax.random.uniform(jax.random.fold_in(key, 103), (H,), jnp.float32, -0.2, 0.2))
    slow_base = jnp.exp(jax.random.uniform(jax.random.fold_in(key, 104), (H,), jnp.float32, math.log(0.3), math.log(1.2))) / TOKENS
    base_rate = jnp.where(quick_heads, fast_base, slow_base)
    return (quick_heads, base_rate, device_factor)


def draw_log_gate(key, part):
    quick_heads, base_rate, device_factor = gate_parts(key)
    jitter = jnp.exp(jax.random.uniform(jax.random.fold_in(key, 105), (H, TOKENS), jnp.float32, -0.7, 0.7))
    rates_every_head = jnp.minimum(base_rate[:, None] * device_factor * jitter, 0.5)
    spots = jax.random.randint(jax.random.fold_in(key, 106), (4,), 0, TOKENS)
    segment_depth = jax.random.uniform(jax.random.fold_in(key, 107), (H, 4), jnp.float32, math.log(0.5), math.log(0.8))
    position_table = (jnp.arange(TOKENS)[:, None] == spots[None, :]).astype(jnp.float32)
    segment_runs = jnp.dot(segment_depth, position_table.T)
    return -rates_every_head + jnp.where(quick_heads[:, None], 0.0, segment_runs)


def draw_beta_rate(key, part):
    quick_heads, base_rate, device_factor = gate_parts(key)
    fast_beta = jnp.exp(jax.random.uniform(jax.random.fold_in(key, 108), (H, TOKENS), jnp.float32, math.log(0.1), math.log(0.9)))
    slow_jitter = jnp.exp(jax.random.uniform(jax.random.fold_in(key, 109), (H, TOKENS), jnp.float32, math.log(0.5), math.log(2.0)))
    slow_beta = K / TOKENS * device_factor * slow_jitter
    return jnp.minimum(jnp.where(quick_heads[:, None], fast_beta, slow_beta), 0.9)


def levels(rng, shape, pieces, low, high):
    def one(axis_at, shards_of):
        steps = jax.random.uniform(jax.random.fold_in(jax.random.fold_in(rng, 6), axis_at), (shards_of,), jnp.float32, low / len(pieces), high / len(pieces))
        return jnp.repeat(jnp.exp(steps), shape[axis_at] // shards_of).reshape((-1,) + (1,) * (len(shape) - axis_at - 1))

    loudness = one(*pieces[0])
    for cut in pieces[1:]:
        loudness = loudness * one(*cut)
    return loudness


def bell_draw(rng, shape, scale, reach, shards=(), kind=jnp.bfloat16):
    loudness = levels(rng, shape, shards, -0.22, 0.18) if shards else 1.0
    entries = jax.random.normal(rng, shape, jnp.float32) * scale * loudness
    return jnp.minimum(jnp.maximum(entries, -reach), reach).astype(kind)


def setup_inputs(seed: int = 0) -> dict:
    key_of = jax.random.split(jax.random.key(seed), 6)
    return {
        "queries": bell_draw(key_of[0], (TOKENS, H, K), 1.0, 6.0, ((0, 256),)),
        "key_rows": bell_draw(key_of[1], (TOKENS, H, K), 1.0, 6.0, ((0, 256),)),
        "value_rows": bell_draw(key_of[2], (TOKENS, H, V), 1.0, 6.0, ((0, 256),)),
        "log_gate": draw_log_gate(jax.random.fold_in(key_of[5], 71), 0),
        "beta_rate": draw_beta_rate(jax.random.fold_in(key_of[5], 71), 0),
    }


EXACT_MATMUL = lax.Precision.HIGHEST

def unit_rows(vectors):
    wide = vectors.astype(jnp.float32)
    return wide / jnp.sqrt(lax.optimization_barrier(jnp.sum(wide * wide, axis=-1, keepdims=True)) + 1e-06)

def invert_unit_lower(strict):
    order_len = strict.shape[-1]
    identity = jnp.eye(order_len, dtype=strict.dtype)
    powered = -strict
    inverse = identity + powered
    span_len = 2
    while span_len < order_len:
        powered = jnp.einsum('hij,hjk->hik', powered, powered, precision=EXACT_MATMUL)
        inverse = inverse + jnp.einsum('hij,hjk->hik', inverse, powered, precision=EXACT_MATMUL)
        span_len = span_len * 2
    return inverse

def stretch_terms(q_head, k_head, v_head, gates, betas):
    order_len = gates.shape[1]
    rows_idx = lax.broadcasted_iota(jnp.int32, (order_len, order_len), 0)
    cols_idx = lax.broadcasted_iota(jnp.int32, (order_len, order_len), 1)
    lower_incl = rows_idx >= cols_idx
    lower_strict = rows_idx > cols_idx
    cum_log = jnp.cumsum(gates, axis=1)
    gaps_log = cum_log[:, :, None] - cum_log[:, None, :]
    decay_mask = jnp.where(lower_incl, jnp.exp(jnp.where(lower_incl, gaps_log, 0.0)), 0.0)
    key_gram = jnp.einsum('hik,hjk->hij', k_head, k_head, precision=EXACT_MATMUL)
    strict = jnp.where(lower_strict, betas[:, :, None] * key_gram, 0.0)
    inv_plain = invert_unit_lower(strict)
    inv_decay = inv_plain * decay_mask
    w_plain = jnp.einsum('hij,hjk->hik', inv_plain, betas[:, :, None] * k_head, precision=EXACT_MATMUL)
    decayed_weight = jnp.exp(cum_log)[:, :, None] * w_plain
    update_basis = jnp.einsum('hij,hjv->hiv', inv_decay, betas[:, :, None] * v_head, precision=EXACT_MATMUL)
    scores = jnp.einsum('hik,hjk->hij', q_head, k_head, precision=EXACT_MATMUL) * decay_mask
    gated_query = jnp.exp(cum_log)[:, :, None] * q_head
    return (cum_log, w_plain, decayed_weight, update_basis, scores, gated_query)

def advance_stretch(passed_state, stretch_parts, k_head):
    cum_log, w_plain, decayed_weight, update_basis, scores, gated_query = stretch_parts
    triangular_solve = update_basis - jnp.einsum('rzi,rib->rzb', decayed_weight, passed_state, precision=EXACT_MATMUL)
    segment_output = jnp.einsum('rzi,rib->rzb', gated_query, passed_state, precision=EXACT_MATMUL)
    segment_output = segment_output + jnp.einsum('hij,hjv->hiv', scores, triangular_solve, precision=EXACT_MATMUL)
    final_log = cum_log[:, -1]
    trailing_keys = jnp.exp(final_log[:, None] - cum_log)[:, :, None] * k_head
    following_state = jnp.exp(final_log)[:, None, None] * passed_state
    following_state = following_state + jnp.einsum('atb,atm->abm', trailing_keys, triangular_solve, precision=EXACT_MATMUL)
    return (segment_output, following_state)

def reference(queries, key_rows, value_rows, log_gate, beta_rate):
    stretch_count = TOKENS // STRETCH
    q_blocks = queries.reshape(stretch_count, STRETCH, H, K)
    k_blocks = key_rows.reshape(stretch_count, STRETCH, H, K)
    v_blocks = value_rows.reshape(stretch_count, STRETCH, H, V)
    g_blocks = jnp.transpose(log_gate.reshape(H, stretch_count, STRETCH), (1, 0, 2))
    b_blocks = jnp.transpose(beta_rate.reshape(H, stretch_count, STRETCH), (1, 0, 2))

    def step_stretch(passed_state, blocks):
        q_part, k_part, v_part, gates, betas = blocks
        q_head = jnp.transpose(unit_rows(q_part), (1, 0, 2))
        k_head = jnp.transpose(unit_rows(k_part), (1, 0, 2))
        v_head = jnp.transpose(v_part.astype(jnp.float32), (1, 0, 2))
        stretch_parts = stretch_terms(q_head, k_head, v_head, gates, betas)
        segment_output, following_state = advance_stretch(passed_state, stretch_parts, k_head)
        return (following_state, jnp.transpose(segment_output, (1, 0, 2)).astype(jnp.bfloat16))
    zero_state = jnp.zeros((H, K, V), jnp.float32)
    final_state, stretch_outs = lax.scan(step_stretch, zero_state, (q_blocks, k_blocks, v_blocks, g_blocks, b_blocks))
    return stretch_outs.reshape(TOKENS, H, V)
```

```python
import functools

import jax
import jax.numpy as jnp
from jax import lax
from jax.experimental import pallas as pl
from jax.experimental.pallas import tpu as pltpu
from jax.sharding import Mesh
from jax.sharding import PartitionSpec as P

GRP_SEQ = ("grp", "seq_0", "seq_1", "seq_2")
MESH = pl.DeviceIdType.MESH
F32 = jnp.float32
BF16 = jnp.bfloat16

T = 128
K = 128
V = 256
H = 8
HH = 4
Q = 64
ROWS = V + K


def dot(a, b):
    return lax.dot_general(a, b, (((1,), (0,)), ((), ())), preferred_element_type=F32)


def dot_nt(a, b):
    return lax.dot_general(a, b, (((1,), (1,)), ((), ())), preferred_element_type=F32)


def split(x):
    high = x.astype(BF16)
    low = (x - high.astype(F32)).astype(BF16)
    return high, low


def side(x):
    return jnp.concatenate(split(x), axis=1)


def fold(wide):
    half = wide.shape[1] // 2
    return wide[:, :half] + wide[:, half:]


def weights(w):
    pair = side(w)
    return jnp.concatenate([pair, pair], axis=0)


def mm(x, w):
    return fold(dot(side(x), weights(w)))


def mm_nt(x, y):
    wide = side(x)
    high, low = split(y)
    return dot_nt(wide, jnp.concatenate([high, high], axis=1)) + dot_nt(
        wide, jnp.concatenate([low, low], axis=1)
    )


def local_kernel(
    q_ref, k_ref, v_ref, lg_ref, be_ref, m_ref, eq_ref, lo_ref, qf, kf, vf0, vf1
):
    kf[...] = k_ref[...].astype(F32).reshape(T * H, K)
    vf0[...] = v_ref[:, :, :K].astype(F32).reshape(T * H, K)
    vf1[...] = v_ref[:, :, K:].astype(F32).reshape(T * H, K)
    qf[...] = q_ref[...].astype(F32).reshape(T * H, K)
    rows_idx = lax.broadcasted_iota(jnp.int32, (T, T), 0)
    cols_idx = lax.broadcasted_iota(jnp.int32, (T, T), 1)
    differ = rows_idx ^ cols_idx
    upper = rows_idx < cols_idx
    upper_incl = rows_idx <= cols_idx
    lower_incl = rows_idx >= cols_idx
    eye = (rows_idx == cols_idx).astype(F32)
    beta = be_ref[...]
    cum = jnp.dot(
        lg_ref[...],
        upper_incl.astype(F32),
        precision=lax.Precision.HIGHEST,
        preferred_element_type=F32,
    )

    heads = range(H)
    key = [kf[pl.ds(h, T, stride=H), :] for h in heads]
    key_b = [key[h].astype(BF16) for h in heads]
    key_t = [key[h].T for h in heads]
    squares = jnp.concatenate(
        [jnp.sum(key_t[h] * key_t[h], axis=0, keepdims=True) for h in heads], axis=0
    )
    key_tb = [key_t[h].astype(BF16) for h in heads]
    rk = 1.0 / jnp.sqrt(squares + 1e-06)
    columns = jnp.concatenate([rk, beta, cum, jnp.zeros((T - 3 * H, T), F32)], axis=0).T
    rk_col = [columns[:, h : h + 1] for h in heads]
    be_col = [columns[:, H + h : H + h + 1] for h in heads]
    cum_col = [columns[:, 2 * H + h : 2 * H + h + 1] for h in heads]
    rk_row = [rk[h : h + 1, :] for h in heads]
    be_row = [beta[h : h + 1, :] for h in heads]
    cum_row = [cum[h : h + 1, :] for h in heads]

    strict = [
        jnp.where(
            upper, dot_nt(key_b[h], key_b[h]) * rk_col[h] * (be_row[h] * rk_row[h]), 0.0
        )
        for h in heads
    ]
    inverse = [eye - jnp.where(differ == 1, strict[h], 0.0) for h in heads]
    span = 2
    while span < T:
        level = (differ >= span) & (differ < 2 * span)
        left = [mm(inverse[h], jnp.where(level, strict[h], 0.0)) for h in heads]
        inverse = [inverse[h] - mm(left[h], inverse[h]) for h in heads]
        span = span * 2

    for h in heads:
        gap = jnp.where(upper_incl, cum_row[h] - cum_col[h], 0.0)
        decay_t = jnp.where(upper_incl, jnp.exp(gap), 0.0)
        value_t = jnp.concatenate(
            [vf0[pl.ds(h, T, stride=H), :].T, vf1[pl.ds(h, T, stride=H), :].T], axis=0
        ).astype(BF16)
        w_t = fold(dot(key_tb[h], side(inverse[h] * (be_col[h] * rk_col[h]))))
        u_t = fold(dot(value_t, side(inverse[h] * decay_t * be_col[h])))
        last = cum[h : h + 1, T - 1 : T]
        into = jnp.concatenate(
            [
                u_t * (rk_row[h] * jnp.exp(last - cum_row[h])),
                w_t * (rk_row[h] * -jnp.exp(last)),
            ],
            axis=0,
        )
        moved = dot(side(into), jnp.concatenate([key_b[h], key_b[h]], axis=0))
        m_ref[h, :V, :] = moved[:V]
        m_ref[h, V:, :] = moved[V:] + eye * jnp.exp(last)

        query = qf[pl.ds(h, T, stride=H), :]
        rq = 1.0 / jnp.sqrt(jnp.sum(query * query, axis=1, keepdims=True) + 1e-06)
        seen = jnp.where(
            lower_incl, dot_nt(query.astype(BF16), key_b[h]) * rq * rk_row[h], 0.0
        )
        gap = jnp.where(lower_incl, cum_col[h] - cum_row[h], 0.0)
        eq_ref[h] = jnp.exp(cum_col[h]) * (query * rq - mm_nt(seen, w_t))
        lo_ref[h] = mm_nt(seen * jnp.exp(gap), u_t)


def joined(earlier, later):
    top = later.shape[0] - K
    moved = mm(earlier, later[top:])
    return jnp.concatenate([moved[:top] + later[:top], moved[top:]], axis=0)


def entered(state, before):
    top = before.shape[0] - K
    return mm(state, before[top:]) + before[:top]


def scan_kernel(
    m_ref,
    s_ref,
    pair,
    chip,
    row,
    row_10,
    row_210,
    row_all,
    y_send,
    y_buf,
    z_in,
    z_out,
    r_send,
    r_buf,
    x_send,
    x_buf,
    c_send,
    full,
    core_sem,
    xa_sem,
    ya_sem,
    z_sem,
    yb_sem,
    xb_sem,
    back_sem,
):
    y = lax.axis_index("seq_0")
    x = lax.axis_index("seq_1")
    c = lax.axis_index("seq_2")
    z = lax.axis_index("grp")
    planes = lax.axis_size("grp")

    def turn(at, o):
        return lax.rem(at + o + 4, 4)

    barrier = pltpu.get_barrier_semaphore()
    peers = [{"seq_2": 1 - c}]
    peers += [{"seq_1": turn(x, o)} for o in (1, 2, 3)]
    peers += [{"seq_0": turn(y, o)} for o in (1, 2, 3)]
    peers += [{"grp": lax.rem(z + 1, planes)}, {"grp": lax.rem(z + planes - 1, planes)}]
    for peer in peers:
        pl.semaphore_signal(barrier, inc=1, device_id=peer, device_id_type=MESH)
    pl.semaphore_wait(barrier, len(peers))

    def copy(src, dst, sem, o, peer):
        return pltpu.make_async_remote_copy(
            src_ref=src,
            dst_ref=dst,
            send_sem=sem.at[0, o],
            recv_sem=sem.at[1, o],
            device_id=peer,
            device_id_type=MESH,
        )

    started = []

    order = (2, 1, 3, 0)
    swaps = {}
    for o in order:
        j = turn(x, o)
        swaps[o] = copy(
            m_ref.at[HH * (1 - c) + j], pair.at[c, j], core_sem, o, {"seq_2": 1 - c}
        )
        swaps[o].start()
        started.append(swaps[o])
    for o in order:
        j = turn(x, o)
        pair[c, j] = m_ref[HH * c + j]
    sends = {}
    for o in order:
        j = turn(x, o)
        swaps[o].wait_recv()
        both = joined(pair[0, j], pair[1, j])
        if o == 0:
            row[x] = both
        else:
            chip[o] = both
            sends[o] = copy(chip.at[o], row.at[x], xa_sem, o, {"seq_1": j})
            sends[o].start()
            started.append(sends[o])
    for o in (1, 3, 2):
        sends[o].wait_recv()

    row_10[...] = joined(row[0], row[1])
    row_32 = joined(row[2], row[3])
    row_all[...] = joined(row_10[...], row_32)

    sends = {}
    for o in (2, 1, 3):
        to = turn(y, o)
        y_send[o, :Q, :] = row_all[pl.ds(pl.multiple_of(to * Q, Q), Q), :]
        y_send[o, Q:, :] = row_all[V:, :]
        sends[o] = copy(y_send.at[o], y_buf.at[y], ya_sem, o, {"seq_0": to})
        sends[o].start()
        started.append(sends[o])
    y_buf[y, :Q, :] = row_all[pl.ds(pl.multiple_of(y * Q, Q), Q), :]
    y_buf[y, Q:, :] = row_all[V:, :]
    row_210[...] = joined(row_10[...], row[2])
    for o in (1, 3, 2):
        sends[o].wait_recv()
    plane_10 = joined(y_buf[0], y_buf[1])
    plane_32 = joined(y_buf[2], y_buf[3])
    plane = joined(plane_10, plane_32)

    hop = copy(z_out, z_in, z_sem, 0, {"grp": lax.rem(z + 1, planes)})

    @pl.when(z == 0)
    def _():
        z_in[...] = jnp.zeros_like(z_in)

    @pl.when(z > 0)
    def _():
        hop.wait_recv()

    state = z_in[...]

    @pl.when(z < planes - 1)
    def _():
        z_out[...] = entered(state, plane)
        hop.start()

    plane_210 = joined(plane_10, y_buf[2])
    r_send[0] = state
    r_send[1] = entered(state, y_buf[0])
    r_send[2] = entered(state, plane_10)
    r_send[3] = entered(state, plane_210)
    mine = pl.ds(pl.multiple_of(y * Q, Q), Q)
    sends = {}
    for o in (2, 1, 3):
        to = turn(y, o)
        sends[o] = copy(r_send.at[to], r_buf.at[mine], yb_sem, o, {"seq_0": to})
        sends[o].start()
        started.append(sends[o])
    r_buf[mine, :] = r_send[y]
    for o in (1, 3, 2):
        sends[o].wait_recv()

    state = r_buf[...]
    x_send[0] = state
    x_send[1] = entered(state, row[0])
    x_send[2] = entered(state, row_10[...])
    x_send[3] = entered(state, row_210[...])
    sends = {}
    for o in (2, 1, 3):
        to = turn(x, o)
        sends[o] = copy(x_send.at[to], x_buf.at[x], xb_sem, o, {"seq_1": to})
        sends[o].start()
        started.append(sends[o])
    x_buf[x] = x_send[x]

    swaps = []
    for o in (0, 1, 3, 2):
        j = turn(x, -o)
        if o > 0:
            sends[o].wait_recv()
        first = x_buf[j]
        second = entered(first, pair[0, j])
        head = HH * c + j
        full[head] = jnp.where(c == 0, first, second)
        c_send[o] = jnp.where(c == 0, second, first)
        swap = copy(c_send.at[o], full.at[head], back_sem, o, {"seq_2": 1 - c})
        swap.start()
        started.append(swap)
        swaps.append(swap)
    for swap in swaps:
        swap.wait_recv()
    s_ref[...] = full[...]

    for sent in started:
        sent.wait_send()

    @pl.when(z < planes - 1)
    def _():
        hop.wait_send()


def final_kernel(eq_ref, lo_ref, s_ref, o_ref, of0, of1):
    for h in range(H):
        both = lo_ref[h] + mm_nt(eq_ref[h], s_ref[h])
        of0[pl.ds(h, T, stride=H), :] = both[:, :K]
        of1[pl.ds(h, T, stride=H), :] = both[:, K:]
    o_ref[:, :, :K] = of0[...].reshape(T, H, K).astype(BF16)
    o_ref[:, :, K:] = of1[...].reshape(T, H, K).astype(BF16)


VM = pl.BlockSpec(memory_space=pltpu.VMEM)


def body(queries, key_rows, value_rows, log_gate, beta_rate):
    maps, eff_query, local_out = pl.pallas_call(
        local_kernel,
        out_shape=(
            jax.ShapeDtypeStruct((H, ROWS, K), F32),
            jax.ShapeDtypeStruct((H, T, K), F32),
            jax.ShapeDtypeStruct((H, T, V), F32),
        ),
        in_specs=[VM] * 5,
        out_specs=(VM, VM, VM),
        scratch_shapes=[pltpu.VMEM((T * H, K), F32)] * 4,
        compiler_params=pltpu.CompilerParams(vmem_limit_bytes=48 * 1024 * 1024),
        name="local",
    )(queries, key_rows, value_rows, log_gate, beta_rate)
    dma = pltpu.SemaphoreType.DMA
    states = pl.pallas_call(
        scan_kernel,
        out_shape=jax.ShapeDtypeStruct((H, V, K), F32),
        in_specs=[VM],
        out_specs=VM,
        scratch_shapes=[
            pltpu.VMEM((2, HH, ROWS, K), F32),
            pltpu.VMEM((4, ROWS, K), F32),
            pltpu.VMEM((4, ROWS, K), F32),
            pltpu.VMEM((ROWS, K), F32),
            pltpu.VMEM((ROWS, K), F32),
            pltpu.VMEM((ROWS, K), F32),
            pltpu.VMEM((4, Q + K, K), F32),
            pltpu.VMEM((4, Q + K, K), F32),
            pltpu.VMEM((Q, K), F32),
            pltpu.VMEM((Q, K), F32),
            pltpu.VMEM((4, Q, K), F32),
            pltpu.VMEM((V, K), F32),
            pltpu.VMEM((4, V, K), F32),
            pltpu.VMEM((4, V, K), F32),
            pltpu.VMEM((4, V, K), F32),
            pltpu.VMEM((H, V, K), F32),
            dma((2, 4)),
            dma((2, 4)),
            dma((2, 4)),
            dma((2, 1)),
            dma((2, 4)),
            dma((2, 4)),
            dma((2, 4)),
        ],
        compiler_params=pltpu.CompilerParams(
            collective_id=0, has_side_effects=True, vmem_limit_bytes=48 * 1024 * 1024
        ),
        name="scan",
    )(maps)
    return pl.pallas_call(
        final_kernel,
        out_shape=jax.ShapeDtypeStruct((T, H, V), BF16),
        in_specs=[VM] * 3,
        out_specs=VM,
        scratch_shapes=[pltpu.VMEM((T * H, K), F32)] * 2,
        compiler_params=pltpu.CompilerParams(vmem_limit_bytes=48 * 1024 * 1024),
        name="final",
    )(eff_query, local_out, states)


def solution(mesh):
    finer = Mesh(
        mesh.devices.reshape(4, 4, 2, mesh.shape["grp"]), ("seq_0", "seq_1", "seq_2", "grp")
    )
    placed = (
        P(GRP_SEQ, None, None),
        P(GRP_SEQ, None, None),
        P(GRP_SEQ, None, None),
        P(None, GRP_SEQ),
        P(None, GRP_SEQ),
    )
    return jax.shard_map(
        body, mesh=finer, in_specs=placed, out_specs=P(GRP_SEQ, None, None), check_vma=False
    )
```

```python
import functools

import jax
import jax.numpy as jnp
from jax import lax
from jax.experimental import pallas as pl
from jax.experimental.pallas import tpu as pltpu
from jax.sharding import Mesh
from jax.sharding import PartitionSpec as P

GRP_SEQ = ("grp", "seq_0", "seq_1", "seq_2")
MESH = pl.DeviceIdType.MESH
F32 = jnp.float32
BF16 = jnp.bfloat16

T = 128
K = 128
V = 256
H = 8
HH = 4
Q = 64
ROWS = V + K


def dot(a, b):
    return lax.dot_general(a, b, (((1,), (0,)), ((), ())), preferred_element_type=F32)


def dot_nt(a, b):
    return lax.dot_general(a, b, (((1,), (1,)), ((), ())), preferred_element_type=F32)


def split(x):
    high = x.astype(BF16)
    low = (x - high.astype(F32)).astype(BF16)
    return high, low


def side(x):
    return jnp.concatenate(split(x), axis=1)


def fold(wide):
    half = wide.shape[1] // 2
    return wide[:, :half] + wide[:, half:]


def weights(w):
    pair = side(w)
    return jnp.concatenate([pair, pair], axis=0)


def mm(x, w):
    return fold(dot(side(x), weights(w)))


def mm_nt(x, y):
    wide = side(x)
    high, low = split(y)
    return dot_nt(wide, jnp.concatenate([high, high], axis=1)) + dot_nt(
        wide, jnp.concatenate([low, low], axis=1)
    )


def joined(earlier, later):
    top = later.shape[0] - K
    moved = mm(earlier, later[top:])
    return jnp.concatenate([moved[:top] + later[:top], moved[top:]], axis=0)


def entered(state, before):
    top = before.shape[0] - K
    return mm(state, before[top:]) + before[:top]


def turn(at, o):
    return lax.rem(at + o + 4, 4)


def scan_kernel(
    q_ref,
    k_ref,
    v_ref,
    lg_ref,
    be_ref,
    o_ref,
    q_in,
    k_in,
    v_in,
    lg_in,
    be_in,
    qf,
    kf,
    vf0,
    vf1,
    w_all,
    u_all,
    eff,
    own,
    maps,
    pair,
    chip,
    row,
    row_10,
    row_210,
    row_all,
    y_send,
    y_buf,
    p_send,
    p_buf,
    z_in,
    z_out,
    enter,
    r_send,
    r_buf,
    x_send,
    x_buf,
    c_send,
    full,
    in_sem,
    core_sem,
    xa_sem,
    ya_sem,
    p_sem,
    z_sem,
    yb_sem,
    xb_sem,
    back_sem,
):
    y = lax.axis_index("seq_0")
    x = lax.axis_index("seq_1")
    c = lax.axis_index("seq_2")
    z = lax.axis_index("grp")
    planes = lax.axis_size("grp")
    heads = range(H)

    loads = []
    for i, (src, dst) in enumerate(
        ((k_ref, k_in), (lg_ref, lg_in), (be_ref, be_in), (v_ref, v_in), (q_ref, q_in))
    ):
        loads.append(pltpu.make_async_copy(src, dst, in_sem.at[i]))
        loads[i].start()

    barrier = pltpu.get_barrier_semaphore()
    peers = [{"seq_2": 1 - c}]
    peers += [{"seq_1": turn(x, o)} for o in (1, 2, 3)]
    peers += [{"seq_0": turn(y, o)} for o in (1, 2, 3)]
    peers += [{"grp": lax.rem(z + planes + o, planes)} for o in (1, -1, 2, -2)]
    for peer in peers:
        pl.semaphore_signal(barrier, inc=1, device_id=peer, device_id_type=MESH)

    def copy(src, dst, sem, o, peer):
        return pltpu.make_async_remote_copy(
            src_ref=src,
            dst_ref=dst,
            send_sem=sem.at[0, o],
            recv_sem=sem.at[1, o],
            device_id=peer,
            device_id_type=MESH,
        )

    started = []

    rows_idx = lax.broadcasted_iota(jnp.int32, (T, T), 0)
    cols_idx = lax.broadcasted_iota(jnp.int32, (T, T), 1)
    differ = rows_idx ^ cols_idx
    upper = rows_idx < cols_idx
    upper_incl = rows_idx <= cols_idx
    lower_incl = rows_idx >= cols_idx
    eye = (rows_idx == cols_idx).astype(F32)
    loads[0].wait()
    kf[...] = k_in[...].astype(F32).reshape(T * H, K)
    key = [kf[pl.ds(h, T, stride=H), :] for h in heads]
    key_b = [key[h].astype(BF16) for h in heads]
    key_t = [key[h].T for h in heads]
    squares = jnp.concatenate(
        [jnp.sum(key_t[h] * key_t[h], axis=0, keepdims=True) for h in heads], axis=0
    )
    key_tb = [key_t[h].astype(BF16) for h in heads]
    loads[1].wait()
    loads[2].wait()
    beta = be_in[...]
    cum = jnp.dot(
        lg_in[...],
        upper_incl.astype(F32),
        precision=lax.Precision.HIGHEST,
        preferred_element_type=F32,
    )
    rk = 1.0 / jnp.sqrt(squares + 1e-06)
    columns = jnp.concatenate([rk, beta, cum, jnp.zeros((T - 3 * H, T), F32)], axis=0).T
    rk_col = [columns[:, h : h + 1] for h in heads]
    be_col = [columns[:, H + h : H + h + 1] for h in heads]
    cum_col = [columns[:, 2 * H + h : 2 * H + h + 1] for h in heads]
    rk_row = [rk[h : h + 1, :] for h in heads]
    be_row = [beta[h : h + 1, :] for h in heads]
    cum_row = [cum[h : h + 1, :] for h in heads]
    strict = [
        jnp.where(
            upper, dot_nt(key_b[h], key_b[h]) * rk_col[h] * (be_row[h] * rk_row[h]), 0.0
        )
        for h in heads
    ]
    inverse = [eye - jnp.where(differ == 1, strict[h], 0.0) for h in heads]
    span = 2
    while span < T:
        level = (differ >= span) & (differ < 2 * span)
        left = [mm(inverse[h], jnp.where(level, strict[h], 0.0)) for h in heads]
        inverse = [inverse[h] - mm(left[h], inverse[h]) for h in heads]
        span = span * 2
    loads[3].wait()
    vf0[...] = v_in[:, :, :K].astype(F32).reshape(T * H, K)
    vf1[...] = v_in[:, :, K:].astype(F32).reshape(T * H, K)
    for h in heads:
        gap = jnp.where(upper_incl, cum_row[h] - cum_col[h], 0.0)
        decay_t = jnp.where(upper_incl, jnp.exp(gap), 0.0)
        value_t = jnp.concatenate(
            [vf0[pl.ds(h, T, stride=H), :].T, vf1[pl.ds(h, T, stride=H), :].T], axis=0
        ).astype(BF16)
        w_t = fold(dot(key_tb[h], side(inverse[h] * (be_col[h] * rk_col[h]))))
        u_t = fold(dot(value_t, side(inverse[h] * decay_t * be_col[h])))
        last = cum[h : h + 1, T - 1 : T]
        into = jnp.concatenate(
            [
                u_t * (rk_row[h] * jnp.exp(last - cum_row[h])),
                w_t * (rk_row[h] * -jnp.exp(last)),
            ],
            axis=0,
        )
        moved = dot(side(into), jnp.concatenate([key_b[h], key_b[h]], axis=0))
        maps[h, :V, :] = moved[:V]
        maps[h, V:, :] = moved[V:] + eye * jnp.exp(last)
        w_all[h] = w_t
        u_all[h] = u_t

    pl.semaphore_wait(barrier, len(peers))

    order = (2, 1, 3, 0)
    swaps = {}
    for o in order:
        j = turn(x, o)
        swaps[o] = copy(
            maps.at[HH * (1 - c) + j], pair.at[c, j], core_sem, o, {"seq_2": 1 - c}
        )
        swaps[o].start()
        started.append(swaps[o])
    for o in order:
        j = turn(x, o)
        pair[c, j] = maps[HH * c + j]
    sends = {}
    for o in order:
        j = turn(x, o)
        swaps[o].wait_recv()
        both = joined(pair[0, j], pair[1, j])
        if o == 0:
            row[x] = both
        else:
            chip[o] = both
            sends[o] = copy(chip.at[o], row.at[x], xa_sem, o, {"seq_1": j})
            sends[o].start()
            started.append(sends[o])

    loads[4].wait()
    qf[...] = q_in[...].astype(F32).reshape(T * H, K)
    for h in heads:
        query = qf[pl.ds(h, T, stride=H), :]
        key_h = kf[pl.ds(h, T, stride=H), :].astype(BF16)
        rq = 1.0 / jnp.sqrt(jnp.sum(query * query, axis=1, keepdims=True) + 1e-06)
        seen = jnp.where(
            lower_incl, dot_nt(query.astype(BF16), key_h) * rq * rk_row[h], 0.0
        )
        gap = jnp.where(lower_incl, cum_col[h] - cum_row[h], 0.0)
        eff[h] = jnp.exp(cum_col[h]) * (query * rq - mm_nt(seen, w_all[h]))
        own[h] = mm_nt(seen * jnp.exp(gap), u_all[h])

    for o in (1, 3, 2):
        sends[o].wait_recv()

    row_10[...] = joined(row[0], row[1])
    row_32 = joined(row[2], row[3])
    row_all[...] = joined(row_10[...], row_32)

    sends = {}
    for o in (2, 1, 3):
        to = turn(y, o)
        y_send[o, :Q, :] = row_all[pl.ds(pl.multiple_of(to * Q, Q), Q), :]
        y_send[o, Q:, :] = row_all[V:, :]
        sends[o] = copy(y_send.at[o], y_buf.at[y], ya_sem, o, {"seq_0": to})
        sends[o].start()
        started.append(sends[o])
    y_buf[y, :Q, :] = row_all[pl.ds(pl.multiple_of(y * Q, Q), Q), :]
    y_buf[y, Q:, :] = row_all[V:, :]
    row_210[...] = joined(row_10[...], row[2])
    for o in (1, 3, 2):
        sends[o].wait_recv()
    plane_10 = joined(y_buf[0], y_buf[1])
    plane_32 = joined(y_buf[2], y_buf[3])
    plane = joined(plane_10, plane_32)

    odd = lax.rem(z, 2) == 1
    next_one = {"grp": lax.rem(z + 1, planes)}
    give_state = copy(p_send.at[pl.ds(0, Q)], p_buf.at[pl.ds(0, Q)], p_sem, 0, next_one)
    give_trans = copy(p_send.at[pl.ds(Q, K)], p_buf.at[pl.ds(Q, K)], p_sem, 1, next_one)
    jump = copy(z_out, z_in, z_sem, 0, {"grp": lax.rem(z + 2, planes)})
    step = copy(z_out, z_in, z_sem, 1, next_one)

    @pl.when(jnp.logical_not(odd))
    def _():
        p_send[...] = plane
        give_state.start()
        give_trans.start()

    plane_210 = joined(plane_10, y_buf[2])

    @pl.when(z == 0)
    def _():
        enter[...] = jnp.zeros_like(enter)

    @pl.when(z == 1)
    def _():
        give_state.wait_recv()
        z_out[...] = entered(p_buf[:Q, :], plane)
        jump.start()
        step.start()
        enter[...] = p_buf[:Q, :]
        give_trans.wait_recv()

    @pl.when(odd & (z > 1))
    def _():
        give_state.wait_recv()
        give_trans.wait_recv()
        two = joined(p_buf[...], plane)
        jump.wait_recv()

        @pl.when(z < planes - 1)
        def _():
            z_out[...] = entered(z_in[...], two)

            @pl.when(z < planes - 2)
            def _():
                jump.start()

            step.start()

        enter[...] = entered(z_in[...], p_buf[...])

    @pl.when(jnp.logical_not(odd) & (z > 0))
    def _():
        step.wait_recv()
        enter[...] = z_in[...]

    state = enter[...]
    r_send[0] = state
    r_send[1] = entered(state, y_buf[0])
    r_send[2] = entered(state, plane_10)
    r_send[3] = entered(state, plane_210)
    mine = pl.ds(pl.multiple_of(y * Q, Q), Q)
    sends = {}
    for o in (2, 1, 3):
        to = turn(y, o)
        sends[o] = copy(r_send.at[to], r_buf.at[mine], yb_sem, o, {"seq_0": to})
        sends[o].start()
        started.append(sends[o])
    r_buf[mine, :] = r_send[y]
    arrivals = {1: [], 2: [], 3: []}
    for o in (0, 1, 3, 2):
        if o > 0:
            sends[o].wait_recv()
        part = pl.ds(pl.multiple_of(turn(y, -o) * Q, Q), Q)
        state = r_buf[part, :]
        x_send[0, part, :] = state
        x_send[1, part, :] = mm(state, row[0, V:, :]) + row[0, part, :]
        x_send[2, part, :] = mm(state, row_10[V:, :]) + row_10[part, :]
        x_send[3, part, :] = mm(state, row_210[V:, :]) + row_210[part, :]
        for a in (2, 1, 3):
            to = turn(x, a)
            sent = copy(
                x_send.at[to, part], x_buf.at[x, part], xb_sem, 4 * a + o, {"seq_1": to}
            )
            sent.start()
            started.append(sent)
            arrivals[a].append(sent)
        x_buf[x, part, :] = x_send[x, part, :]

    def read_out(head):
        both = own[head] + mm_nt(eff[head], full[head])
        vf0[pl.ds(head, T, stride=H), :] = both[:, :K]
        vf1[pl.ds(head, T, stride=H), :] = both[:, K:]

    swaps = []
    for a in (0, 1, 3, 2):
        j = turn(x, -a)
        if a > 0:
            for sent in arrivals[a]:
                sent.wait_recv()
        first = x_buf[j]
        second = entered(first, pair[0, j])
        head = HH * c + j
        full[head] = jnp.where(c == 0, first, second)
        c_send[a] = jnp.where(c == 0, second, first)
        swap = copy(c_send.at[a], full.at[head], back_sem, a, {"seq_2": 1 - c})
        swap.start()
        started.append(swap)
        swaps.append((swap, j))
        read_out(head)
    for swap, j in swaps:
        swap.wait_recv()
        read_out(HH * (1 - c) + j)
    o_ref[:, :, :K] = vf0[...].reshape(T, H, K).astype(BF16)
    o_ref[:, :, K:] = vf1[...].reshape(T, H, K).astype(BF16)

    for sent in started:
        sent.wait_send()

    @pl.when(jnp.logical_not(odd))
    def _():
        give_state.wait_send()
        give_trans.wait_send()

    @pl.when(odd & (z < planes - 1))
    def _():
        step.wait_send()

    @pl.when(odd & (z < planes - 2))
    def _():
        jump.wait_send()


def body(*given):
    queries, key_rows, value_rows, log_gate, beta_rate = [pltpu.with_memory_space_constraint(a, pltpu.HBM) for a in given]
    dma = pltpu.SemaphoreType.DMA

    def room(*shape):
        return pltpu.VMEM(shape, F32)

    return pl.pallas_call(
        scan_kernel,
        out_shape=jax.ShapeDtypeStruct((T, H, V), BF16),
        in_specs=[pl.BlockSpec(memory_space=pltpu.HBM)] * 5,
        out_specs=pl.BlockSpec(memory_space=pltpu.VMEM),
        scratch_shapes=[
            pltpu.VMEM((T, H, K), BF16),
            pltpu.VMEM((T, H, K), BF16),
            pltpu.VMEM((T, H, V), BF16),
            room(H, T),
            room(H, T),
            room(T * H, K),
            room(T * H, K),
            room(T * H, K),
            room(T * H, K),
            room(H, K, T),
            room(H, V, T),
            room(H, T, K),
            room(H, T, V),
            room(H, ROWS, K),
            room(2, HH, ROWS, K),
            room(4, ROWS, K),
            room(4, ROWS, K),
            room(ROWS, K),
            room(ROWS, K),
            room(ROWS, K),
            room(4, Q + K, K),
            room(4, Q + K, K),
            room(Q + K, K),
            room(Q + K, K),
            room(Q, K),
            room(Q, K),
            room(Q, K),
            room(4, Q, K),
            room(V, K),
            room(4, V, K),
            room(4, V, K),
            room(4, V, K),
            room(H, V, K),
            dma((5,)),
            dma((2, 4)),
            dma((2, 4)),
            dma((2, 4)),
            dma((2, 2)),
            dma((2, 2)),
            dma((2, 4)),
            dma((2, 16)),
            dma((2, 4)),
        ],
        compiler_params=pltpu.CompilerParams(
            collective_id=0, has_side_effects=True, vmem_limit_bytes=48 * 1024 * 1024
        ),
        name="scan",
    )(queries, key_rows, value_rows, log_gate, beta_rate)


def solution(mesh):
    finer = Mesh(
        mesh.devices.reshape(4, 4, 2, mesh.shape["grp"]), ("seq_0", "seq_1", "seq_2", "grp")
    )
    placed = (
        P(GRP_SEQ, None, None),
        P(GRP_SEQ, None, None),
        P(GRP_SEQ, None, None),
        P(None, GRP_SEQ),
        P(None, GRP_SEQ),
    )
    return jax.shard_map(
        body, mesh=finer, in_specs=placed, out_specs=P(GRP_SEQ, None, None), check_vma=False
    )
```

```python
import functools

import jax
import jax.numpy as jnp
from jax import lax
from jax.experimental import pallas as pl
from jax.experimental.pallas import tpu as pltpu
from jax.sharding import Mesh
from jax.sharding import PartitionSpec as P

GRP_SEQ = ("grp", "seq_0", "seq_1", "seq_2")
MESH = pl.DeviceIdType.MESH
F32 = jnp.float32
BF16 = jnp.bfloat16

T = 128
K = 128
V = 256
H = 8
HH = 4
Q = 64
ROWS = V + K


def dot(a, b):
    return lax.dot_general(a, b, (((1,), (0,)), ((), ())), preferred_element_type=F32)


def dot_nt(a, b):
    return lax.dot_general(a, b, (((1,), (1,)), ((), ())), preferred_element_type=F32)


def split(x):
    high = x.astype(BF16)
    low = (x - high.astype(F32)).astype(BF16)
    return high, low


def side(x):
    return jnp.concatenate(split(x), axis=1)


def fold(wide):
    half = wide.shape[1] // 2
    return wide[:, :half] + wide[:, half:]


def weights(w):
    pair = side(w)
    return jnp.concatenate([pair, pair], axis=0)


def mm(x, w):
    return fold(dot(side(x), weights(w)))


def mm_nt(x, y):
    wide = side(x)
    high, low = split(y)
    return dot_nt(wide, jnp.concatenate([high, high], axis=1)) + dot_nt(
        wide, jnp.concatenate([low, low], axis=1)
    )


def joined(earlier, later):
    top = later.shape[0] - K
    moved = mm(earlier, later[top:])
    return jnp.concatenate([moved[:top] + later[:top], moved[top:]], axis=0)


def entered(state, before):
    top = before.shape[0] - K
    return mm(state, before[top:]) + before[:top]


def turn(at, o):
    return lax.rem(at + o + 4, 4)


def scan_kernel(
    q_ref,
    k_ref,
    v_ref,
    lg_ref,
    be_ref,
    o_ref,
    q_in,
    k_in,
    v_in,
    lg_in,
    be_in,
    qf,
    kf,
    vf0,
    vf1,
    w_all,
    u_all,
    eff,
    own,
    maps,
    pair,
    chip,
    row,
    row_10,
    row_210,
    row_all,
    y_send,
    y_buf,
    p_send,
    p_buf,
    z_in,
    z_out,
    enter,
    r_send,
    r_buf,
    x_send,
    x_buf,
    c_send,
    full,
    in_sem,
    core_sem,
    xa_sem,
    ya_sem,
    p_sem,
    z_sem,
    yb_sem,
    xb_sem,
    back_sem,
):
    y = lax.axis_index("seq_0")
    x = lax.axis_index("seq_1")
    c = lax.axis_index("seq_2")
    z = lax.axis_index("grp")
    planes = lax.axis_size("grp")
    heads = range(H)

    loads = []
    for i, (src, dst) in enumerate(
        ((k_ref, k_in), (lg_ref, lg_in), (be_ref, be_in), (v_ref, v_in), (q_ref, q_in))
    ):
        loads.append(pltpu.make_async_copy(src, dst, in_sem.at[i]))
        loads[i].start()

    barrier = pltpu.get_barrier_semaphore()
    peers = [{"seq_2": 1 - c}]
    peers += [{"seq_1": turn(x, o)} for o in (1, 2, 3)]
    peers += [{"seq_0": turn(y, o)} for o in (1, 2, 3)]
    peers += [{"grp": lax.rem(z + planes + o, planes)} for o in (1, -1, 2, -2)]
    for peer in peers:
        pl.semaphore_signal(barrier, inc=1, device_id=peer, device_id_type=MESH)

    def copy(src, dst, sem, o, peer):
        return pltpu.make_async_remote_copy(
            src_ref=src,
            dst_ref=dst,
            send_sem=sem.at[0, o],
            recv_sem=sem.at[1, o],
            device_id=peer,
            device_id_type=MESH,
        )

    started = []

    rows_idx = lax.broadcasted_iota(jnp.int32, (T, T), 0)
    cols_idx = lax.broadcasted_iota(jnp.int32, (T, T), 1)
    differ = rows_idx ^ cols_idx
    upper = rows_idx < cols_idx
    upper_incl = rows_idx <= cols_idx
    lower_incl = rows_idx >= cols_idx
    eye = (rows_idx == cols_idx).astype(F32)
    loads[0].wait()
    kf[...] = k_in[...].astype(F32).reshape(T * H, K)
    key = [kf[pl.ds(h, T, stride=H), :] for h in heads]
    key_b = [key[h].astype(BF16) for h in heads]
    key_t = [key[h].T for h in heads]
    squares = jnp.concatenate(
        [jnp.sum(key_t[h] * key_t[h], axis=0, keepdims=True) for h in heads], axis=0
    )
    key_tb = [key_t[h].astype(BF16) for h in heads]
    loads[1].wait()
    loads[2].wait()
    beta = be_in[...]
    cum = jnp.dot(
        lg_in[...],
        upper_incl.astype(F32),
        precision=lax.Precision.HIGHEST,
        preferred_element_type=F32,
    )
    rk = 1.0 / jnp.sqrt(squares + 1e-06)
    columns = jnp.concatenate([rk, beta, cum, jnp.zeros((T - 3 * H, T), F32)], axis=0).T
    rk_col = [columns[:, h : h + 1] for h in heads]
    be_col = [columns[:, H + h : H + h + 1] for h in heads]
    cum_col = [columns[:, 2 * H + h : 2 * H + h + 1] for h in heads]
    rk_row = [rk[h : h + 1, :] for h in heads]
    be_row = [beta[h : h + 1, :] for h in heads]
    cum_row = [cum[h : h + 1, :] for h in heads]
    strict = [
        jnp.where(
            upper, dot_nt(key_b[h], key_b[h]) * rk_col[h] * (be_row[h] * rk_row[h]), 0.0
        )
        for h in heads
    ]
    inverse = [eye - jnp.where(differ == 1, strict[h], 0.0) for h in heads]
    span = 2
    while span < T:
        level = (differ >= span) & (differ < 2 * span)
        left = [mm(inverse[h], jnp.where(level, strict[h], 0.0)) for h in heads]
        inverse = [inverse[h] - mm(left[h], inverse[h]) for h in heads]
        span = span * 2
    loads[3].wait()
    vf0[...] = v_in[:, :, :K].astype(F32).reshape(T * H, K)
    vf1[...] = v_in[:, :, K:].astype(F32).reshape(T * H, K)
    for h in heads:
        gap = jnp.where(upper_incl, cum_row[h] - cum_col[h], 0.0)
        decay_t = jnp.where(upper_incl, jnp.exp(gap), 0.0)
        value_t = jnp.concatenate(
            [vf0[pl.ds(h, T, stride=H), :].T, vf1[pl.ds(h, T, stride=H), :].T], axis=0
        ).astype(BF16)
        w_t = fold(dot(key_tb[h], side(inverse[h] * (be_col[h] * rk_col[h]))))
        u_t = fold(dot(value_t, side(inverse[h] * decay_t * be_col[h])))
        last = cum[h : h + 1, T - 1 : T]
        into = jnp.concatenate(
            [
                u_t * (rk_row[h] * jnp.exp(last - cum_row[h])),
                w_t * (rk_row[h] * -jnp.exp(last)),
            ],
            axis=0,
        )
        moved = dot(side(into), jnp.concatenate([key_b[h], key_b[h]], axis=0))
        maps[h, :V, :] = moved[:V]
        maps[h, V:, :] = moved[V:] + eye * jnp.exp(last)
        w_all[h] = w_t
        u_all[h] = u_t

    pl.semaphore_wait(barrier, len(peers))

    order = (2, 1, 3, 0)
    tail = pl.ds(V, K)
    body_rows = pl.ds(0, V)
    swaps = {}
    for i, rows in ((0, tail), (4, body_rows)):
        for o in order:
            j = turn(x, o)
            swaps[i + o] = copy(
                maps.at[HH * (1 - c) + j, rows],
                pair.at[c, j, rows],
                core_sem,
                i + o,
                {"seq_2": 1 - c},
            )
            swaps[i + o].start()
            started.append(swaps[i + o])
    for o in order:
        j = turn(x, o)
        pair[c, j] = maps[HH * c + j]

    def along_x(o, rows, slot):
        sent = copy(
            chip.at[o, rows],
            row.at[x, rows],
            xa_sem,
            5 * (o - 1) + slot,
            {"seq_1": turn(x, o)},
        )
        sent.start()
        started.append(sent)
        return sent

    def quarter(o):
        return pl.ds(pl.multiple_of(turn(y, o) * Q, Q), Q)

    sends = {}
    for o in order:
        j = turn(x, o)
        swaps[o].wait_recv()
        both = mm(pair[0, j, V:, :], pair[1, j, V:, :])
        if o == 0:
            row[x, V:, :] = both
        else:
            chip[o, V:, :] = both
            sends[o, 4] = along_x(o, tail, 4)
    for o in order:
        j = turn(x, o)
        swaps[4 + o].wait_recv()
        both = mm(pair[0, j, :V, :], pair[1, j, V:, :]) + pair[1, j, :V, :]
        if o == 0:
            row[x, :V, :] = both
        else:
            chip[o, :V, :] = both
            sends[o, 2] = along_x(o, quarter(2), 2)
    for part in (1, 3, 0):
        for o in (2, 1, 3):
            sends[o, part] = along_x(o, quarter(part), part)

    loads[4].wait()
    qf[...] = q_in[...].astype(F32).reshape(T * H, K)
    for h in heads:
        query = qf[pl.ds(h, T, stride=H), :]
        key_h = kf[pl.ds(h, T, stride=H), :].astype(BF16)
        rq = 1.0 / jnp.sqrt(jnp.sum(query * query, axis=1, keepdims=True) + 1e-06)
        seen = jnp.where(
            lower_incl, dot_nt(query.astype(BF16), key_h) * rq * rk_row[h], 0.0
        )
        gap = jnp.where(lower_incl, cum_col[h] - cum_row[h], 0.0)
        eff[h] = jnp.exp(cum_col[h]) * (query * rq - mm_nt(seen, w_all[h]))
        own[h] = mm_nt(seen * jnp.exp(gap), u_all[h])

    for o in (1, 3, 2):
        sends[o, 4].wait_recv()
    row_t = [row[k, V:, :] for k in range(4)]
    row_t10 = mm(row_t[0], row_t[1])
    row_t32 = mm(row_t[2], row_t[3])
    row_10[V:, :] = row_t10
    row_all[...] = mm(row_t10, row_t32)
    gives = {}
    for o in (2, 1, 3):
        gives[o] = copy(
            row_all, y_buf.at[y, pl.ds(Q, K)], ya_sem, o, {"seq_0": turn(y, o)}
        )
        gives[o].start()
        started.append(gives[o])
    y_buf[y, Q:, :] = row_all[...]
    weights_1 = weights(row_t[1])
    weights_3 = weights(row_t[3])
    weights_32 = weights(row_t32)
    for part in (2, 1, 3, 0):
        rows = quarter(part)
        for o in (1, 3, 2):
            sends[o, part].wait_recv()
        part_10 = fold(dot(side(row[0, rows, :]), weights_1)) + row[1, rows, :]
        part_32 = fold(dot(side(row[2, rows, :]), weights_3)) + row[3, rows, :]
        row_10[rows, :] = part_10
        total = fold(dot(side(part_10), weights_32)) + part_32
        if part == 0:
            y_buf[y, :Q, :] = total
        else:
            y_send[part] = total
            gives[4 + part] = copy(
                y_send.at[part],
                y_buf.at[y, pl.ds(0, Q)],
                ya_sem,
                4 + part,
                {"seq_0": turn(y, part)},
            )
            gives[4 + part].start()
            started.append(gives[4 + part])
    for o in (1, 3, 2):
        gives[o].wait_recv()
    plane_t = [y_buf[k, Q:, :] for k in range(4)]
    plane_t10 = mm(plane_t[0], plane_t[1])
    plane_t32 = mm(plane_t[2], plane_t[3])
    trans = mm(plane_t10, plane_t32)

    odd = lax.rem(z, 2) == 1
    even = jnp.logical_not(odd)
    next_one = {"grp": lax.rem(z + 1, planes)}
    give_state = copy(p_send.at[pl.ds(0, Q)], p_buf.at[pl.ds(0, Q)], p_sem, 0, next_one)
    give_trans = copy(p_send.at[pl.ds(Q, K)], p_buf.at[pl.ds(Q, K)], p_sem, 1, next_one)
    jump = copy(z_out, z_in, z_sem, 0, {"grp": lax.rem(z + 2, planes)})
    step = copy(z_out, z_in, z_sem, 1, next_one)

    @pl.when(even & (z > 0))
    def _():
        p_send[Q:, :] = trans
        give_trans.start()

    for o in (3, 1, 2):
        gives[4 + o].wait_recv()
    plane_s = [y_buf[k, :Q, :] for k in range(4)]
    plane_s10 = mm(plane_s[0], plane_t[1]) + plane_s[1]
    plane_s32 = mm(plane_s[2], plane_t[3]) + plane_s[3]
    total = mm(plane_s10, plane_t32) + plane_s32

    @pl.when(even)
    def _():
        p_send[:Q, :] = total
        give_state.start()

    row_210[...] = joined(row_10[...], row[2])
    plane_10 = jnp.concatenate([plane_s10, plane_t10], axis=0)
    plane_210 = joined(plane_10, y_buf[2])

    @pl.when(z == 0)
    def _():
        enter[...] = jnp.zeros_like(enter)

    @pl.when(z == 1)
    def _():
        give_state.wait_recv()
        z_out[...] = mm(p_buf[:Q, :], trans) + total
        jump.start()
        step.start()
        enter[...] = p_buf[:Q, :]

    @pl.when(odd & (z > 1))
    def _():
        give_trans.wait_recv()
        two_t = mm(p_buf[Q:, :], trans)
        give_state.wait_recv()
        two_s = mm(p_buf[:Q, :], trans) + total
        jump.wait_recv()

        @pl.when(z < planes - 1)
        def _():
            z_out[...] = mm(z_in[...], two_t) + two_s

            @pl.when(z < planes - 2)
            def _():
                jump.start()

            step.start()

        enter[...] = entered(z_in[...], p_buf[...])

    @pl.when(even & (z > 0))
    def _():
        step.wait_recv()
        enter[...] = z_in[...]

    state = enter[...]
    r_send[0] = state
    r_send[1] = entered(state, y_buf[0])
    r_send[2] = entered(state, plane_10)
    r_send[3] = entered(state, plane_210)
    mine = pl.ds(pl.multiple_of(y * Q, Q), Q)
    sends = {}
    for o in (2, 1, 3):
        to = turn(y, o)
        sends[o] = copy(r_send.at[to], r_buf.at[mine], yb_sem, o, {"seq_0": to})
        sends[o].start()
        started.append(sends[o])
    r_buf[mine, :] = r_send[y]
    arrivals = {1: [], 2: [], 3: []}
    for o in (0, 1, 3, 2):
        if o > 0:
            sends[o].wait_recv()
        part = pl.ds(pl.multiple_of(turn(y, -o) * Q, Q), Q)
        state = r_buf[part, :]
        x_send[0, part, :] = state
        x_send[1, part, :] = mm(state, row[0, V:, :]) + row[0, part, :]
        x_send[2, part, :] = mm(state, row_10[V:, :]) + row_10[part, :]
        x_send[3, part, :] = mm(state, row_210[V:, :]) + row_210[part, :]
        for a in (2, 1, 3):
            to = turn(x, a)
            sent = copy(
                x_send.at[to, part], x_buf.at[x, part], xb_sem, 4 * a + o, {"seq_1": to}
            )
            sent.start()
            started.append(sent)
            arrivals[a].append(sent)
        x_buf[x, part, :] = x_send[x, part, :]

    def read_out(head):
        both = own[head] + mm_nt(eff[head], full[head])
        vf0[pl.ds(head, T, stride=H), :] = both[:, :K]
        vf1[pl.ds(head, T, stride=H), :] = both[:, K:]

    swaps = []
    for a in (0, 1, 3, 2):
        j = turn(x, -a)
        if a > 0:
            for sent in arrivals[a]:
                sent.wait_recv()
        first = x_buf[j]
        second = entered(first, pair[0, j])
        head = HH * c + j
        full[head] = jnp.where(c == 0, first, second)
        c_send[a] = jnp.where(c == 0, second, first)
        swap = copy(c_send.at[a], full.at[head], back_sem, a, {"seq_2": 1 - c})
        swap.start()
        started.append(swap)
        swaps.append((swap, j))
        read_out(head)
    for swap, j in swaps:
        swap.wait_recv()
        read_out(HH * (1 - c) + j)
    o_ref[:, :, :K] = vf0[...].reshape(T, H, K).astype(BF16)
    o_ref[:, :, K:] = vf1[...].reshape(T, H, K).astype(BF16)

    for sent in started:
        sent.wait_send()

    @pl.when(even)
    def _():
        give_state.wait_send()

    @pl.when(even & (z > 0))
    def _():
        give_trans.wait_send()

    @pl.when(odd & (z < planes - 1))
    def _():
        step.wait_send()

    @pl.when(odd & (z < planes - 2))
    def _():
        jump.wait_send()


def body(*given):
    queries, key_rows, value_rows, log_gate, beta_rate = [pltpu.with_memory_space_constraint(a, pltpu.HBM) for a in given]
    dma = pltpu.SemaphoreType.DMA

    def room(*shape):
        return pltpu.VMEM(shape, F32)

    return pl.pallas_call(
        scan_kernel,
        out_shape=jax.ShapeDtypeStruct((T, H, V), BF16),
        in_specs=[pl.BlockSpec(memory_space=pltpu.HBM)] * 5,
        out_specs=pl.BlockSpec(memory_space=pltpu.VMEM),
        scratch_shapes=[
            pltpu.VMEM((T, H, K), BF16),
            pltpu.VMEM((T, H, K), BF16),
            pltpu.VMEM((T, H, V), BF16),
            room(H, T),
            room(H, T),
            room(T * H, K),
            room(T * H, K),
            room(T * H, K),
            room(T * H, K),
            room(H, K, T),
            room(H, V, T),
            room(H, T, K),
            room(H, T, V),
            room(H, ROWS, K),
            room(2, HH, ROWS, K),
            room(4, ROWS, K),
            room(4, ROWS, K),
            room(ROWS, K),
            room(ROWS, K),
            room(K, K),
            room(4, Q, K),
            room(4, Q + K, K),
            room(Q + K, K),
            room(Q + K, K),
            room(Q, K),
            room(Q, K),
            room(Q, K),
            room(4, Q, K),
            room(V, K),
            room(4, V, K),
            room(4, V, K),
            room(4, V, K),
            room(H, V, K),
            dma((5,)),
            dma((2, 8)),
            dma((2, 15)),
            dma((2, 8)),
            dma((2, 2)),
            dma((2, 2)),
            dma((2, 4)),
            dma((2, 16)),
            dma((2, 4)),
        ],
        compiler_params=pltpu.CompilerParams(
            collective_id=0, has_side_effects=True, vmem_limit_bytes=48 * 1024 * 1024
        ),
        name="scan",
    )(queries, key_rows, value_rows, log_gate, beta_rate)


def solution(mesh):
    finer = Mesh(
        mesh.devices.reshape(4, 4, 2, mesh.shape["grp"]), ("seq_0", "seq_1", "seq_2", "grp")
    )
    placed = (
        P(GRP_SEQ, None, None),
        P(GRP_SEQ, None, None),
        P(GRP_SEQ, None, None),
        P(None, GRP_SEQ),
        P(None, GRP_SEQ),
    )
    return jax.shard_map(
        body, mesh=finer, in_specs=placed, out_specs=P(GRP_SEQ, None, None), check_vma=False
    )
```

```python
import functools

import jax
import jax.numpy as jnp
from jax import lax
from jax.experimental import pallas as pl
from jax.experimental.pallas import tpu as pltpu
from jax.sharding import Mesh
from jax.sharding import PartitionSpec as P

GRP_SEQ = ("grp", "seq_0", "seq_1", "seq_2")
MESH = pl.DeviceIdType.MESH
F32 = jnp.float32
BF16 = jnp.bfloat16

T = 128
K = 128
V = 256
H = 8
HH = 4
Q = 64
NEAR = 16
PIECES = 2
ROWS = V + K


def dot(a, b):
    return lax.dot_general(a, b, (((1,), (0,)), ((), ())), preferred_element_type=F32)


def dot_nt(a, b):
    return lax.dot_general(a, b, (((1,), (1,)), ((), ())), preferred_element_type=F32)


def split(x):
    high = x.astype(BF16)
    low = (x - high.astype(F32)).astype(BF16)
    return high, low


def side(x):
    return jnp.concatenate(split(x), axis=1)


def fold(wide):
    half = wide.shape[1] // 2
    return wide[:, :half] + wide[:, half:]


def weights(w):
    pair = side(w)
    return jnp.concatenate([pair, pair], axis=0)


def mm(x, w):
    count = x.shape[0]
    if count > Q:
        return fold(dot(side(x), weights(w)))
    both = fold(dot(jnp.concatenate(split(x), axis=0), side(w)))
    return both[:count] + both[count:]


def mm_nt(x, y):
    wide = side(x)
    high, low = split(y)
    return dot_nt(wide, jnp.concatenate([high, high], axis=1)) + dot_nt(
        wide, jnp.concatenate([low, low], axis=1)
    )


def joined(earlier, later):
    top = later.shape[0] - K
    moved = mm(earlier, later[top:])
    return jnp.concatenate([moved[:top] + later[:top], moved[top:]], axis=0)


def entered(state, before):
    top = before.shape[0] - K
    return mm(state, before[top:]) + before[:top]


def turn(at, o):
    return lax.rem(at + o + 4, 4)


def scan_kernel(
    q_ref,
    k_ref,
    v_ref,
    lg_ref,
    be_ref,
    o_ref,
    q_in,
    k_in,
    v_in,
    lg_in,
    be_in,
    qf,
    kf,
    vf0,
    vf1,
    w_all,
    u_all,
    eff,
    own,
    maps,
    pair,
    chip,
    row,
    row_10,
    row_210,
    row_all,
    y_send,
    y_buf,
    p_send,
    p_buf,
    h_send,
    h_buf,
    z_in,
    z_out,
    enter,
    r_send,
    r_buf,
    x_send,
    x_buf,
    c_send,
    full,
    in_sem,
    core_sem,
    xa_sem,
    ya_sem,
    p_sem,
    h_sem,
    z_sem,
    yb_sem,
    xb_sem,
    back_sem,
):
    y = lax.axis_index("seq_0")
    x = lax.axis_index("seq_1")
    c = lax.axis_index("seq_2")
    z = lax.axis_index("grp")
    planes = lax.axis_size("grp")
    heads = range(H)

    loads = []
    for i, (src, dst) in enumerate(
        ((k_ref, k_in), (lg_ref, lg_in), (be_ref, be_in), (v_ref, v_in), (q_ref, q_in))
    ):
        loads.append(pltpu.make_async_copy(src, dst, in_sem.at[i]))
        loads[i].start()

    barrier = pltpu.get_barrier_semaphore()
    peers = [{"seq_2": 1 - c}]
    peers += [{"seq_1": turn(x, o)} for o in (1, 2, 3)]
    peers += [{"seq_0": turn(y, o)} for o in (1, 2, 3)]
    peers += [{"grp": lax.rem(z + planes + o, planes)} for o in (1, -1, 2, -2, 3, -3, 4)]
    for peer in peers:
        pl.semaphore_signal(barrier, inc=1, device_id=peer, device_id_type=MESH)

    def copy(src, dst, sem, o, peer):
        return pltpu.make_async_remote_copy(
            src_ref=src,
            dst_ref=dst,
            send_sem=sem.at[0, o],
            recv_sem=sem.at[1, o],
            device_id=peer,
            device_id_type=MESH,
        )

    started = []

    rows_idx = lax.broadcasted_iota(jnp.int32, (T, T), 0)
    cols_idx = lax.broadcasted_iota(jnp.int32, (T, T), 1)
    differ = rows_idx ^ cols_idx
    upper = rows_idx < cols_idx
    upper_incl = rows_idx <= cols_idx
    lower_incl = rows_idx >= cols_idx
    eye = (rows_idx == cols_idx).astype(F32)
    loads[0].wait()
    kf[...] = k_in[...].astype(F32).reshape(T * H, K)
    key = [kf[pl.ds(h, T, stride=H), :] for h in heads]
    key_b = [key[h].astype(BF16) for h in heads]
    key_t = [key[h].T for h in heads]
    squares = jnp.concatenate(
        [jnp.sum(key_t[h] * key_t[h], axis=0, keepdims=True) for h in heads], axis=0
    )
    key_tb = [key_t[h].astype(BF16) for h in heads]
    loads[1].wait()
    loads[2].wait()
    beta = be_in[...]
    cum = jnp.dot(
        lg_in[...],
        upper_incl.astype(F32),
        precision=lax.Precision.HIGHEST,
        preferred_element_type=F32,
    )
    rk = 1.0 / jnp.sqrt(squares + 1e-06)
    columns = jnp.concatenate([rk, beta, cum, jnp.zeros((T - 3 * H, T), F32)], axis=0).T
    rk_col = [columns[:, h : h + 1] for h in heads]
    be_col = [columns[:, H + h : H + h + 1] for h in heads]
    cum_col = [columns[:, 2 * H + h : 2 * H + h + 1] for h in heads]
    rk_row = [rk[h : h + 1, :] for h in heads]
    be_row = [beta[h : h + 1, :] for h in heads]
    cum_row = [cum[h : h + 1, :] for h in heads]
    strict = [
        jnp.where(
            upper, dot_nt(key_b[h], key_b[h]) * rk_col[h] * (be_row[h] * rk_row[h]), 0.0
        )
        for h in heads
    ]
    near = [jnp.where(differ < NEAR, strict[h], 0.0) for h in heads]
    inverse = [eye - near[h] for h in heads]
    power = [mm(near[h], near[h]) for h in heads]
    reach = 4
    while reach < NEAR:
        grown = [
            mm(jnp.concatenate([inverse[h], power[h]], axis=0), power[h]) for h in heads
        ]
        inverse = [inverse[h] + grown[h][:T] for h in heads]
        power = [grown[h][T:] for h in heads]
        reach = reach * 2
    inverse = [inverse[h] + mm(inverse[h], power[h]) for h in heads]
    span = NEAR
    while span < T:
        level = (differ >= span) & (differ < 2 * span)
        starts = range(0, T, 2 * span)
        left = [
            mm(
                jnp.concatenate([inverse[h][a : a + span] for a in starts], axis=0),
                jnp.where(level, strict[h], 0.0),
            )
            for h in heads
        ]
        change = [mm(left[h], inverse[h]) for h in heads]
        inverse = [
            jnp.concatenate(
                [
                    piece
                    for i, a in enumerate(starts)
                    for piece in (
                        inverse[h][a : a + span] - change[h][i * span : (i + 1) * span],
                        inverse[h][a + span : a + 2 * span],
                    )
                ],
                axis=0,
            )
            for h in heads
        ]
        span = span * 2
    twice = [jnp.concatenate([key_b[h], key_b[h]], axis=0) for h in heads]
    last = [cum[h : h + 1, T - 1 : T] for h in heads]
    for h in heads:
        w_t = fold(dot(key_tb[h], side(inverse[h] * (be_col[h] * rk_col[h]))))
        moved = dot(side(w_t * (rk_row[h] * -jnp.exp(last[h]))), twice[h])
        maps[h, V:, :] = moved + eye * jnp.exp(last[h])
        w_all[h] = w_t

    pl.semaphore_wait(barrier, len(peers))

    order = (2, 1, 3, 0)
    tail = pl.ds(V, K)
    body_rows = pl.ds(0, V)
    swaps = {}

    def swap_cores(i, o, rows):
        j = turn(x, o)
        swaps[i + o] = copy(
            maps.at[HH * (1 - c) + j, rows],
            pair.at[c, j, rows],
            core_sem,
            i + o,
            {"seq_2": 1 - c},
        )
        swaps[i + o].start()
        started.append(swaps[i + o])

    for o in order:
        swap_cores(0, o, tail)
    loads[3].wait()
    vf0[...] = v_in[:, :, :K].astype(F32).reshape(T * H, K)
    vf1[...] = v_in[:, :, K:].astype(F32).reshape(T * H, K)
    for h in heads:
        gap = jnp.where(upper_incl, cum_row[h] - cum_col[h], 0.0)
        decay_t = jnp.where(upper_incl, jnp.exp(gap), 0.0)
        value_t = jnp.concatenate(
            [vf0[pl.ds(h, T, stride=H), :].T, vf1[pl.ds(h, T, stride=H), :].T], axis=0
        ).astype(BF16)
        u_t = fold(dot(value_t, side(inverse[h] * decay_t * be_col[h])))
        scaled = u_t * (rk_row[h] * jnp.exp(last[h] - cum_row[h]))
        maps[h, :V, :] = dot(side(scaled), twice[h])
        u_all[h] = u_t
    for o in order:
        swap_cores(4, o, body_rows)
    for o in order:
        j = turn(x, o)
        pair[c, j] = maps[HH * c + j]

    def along_x(o, rows, slot):
        sent = copy(
            chip.at[o, rows],
            row.at[x, rows],
            xa_sem,
            5 * (o - 1) + slot,
            {"seq_1": turn(x, o)},
        )
        sent.start()
        started.append(sent)
        return sent

    def quarter(o):
        return pl.ds(pl.multiple_of(turn(y, o) * Q, Q), Q)

    sends = {}
    for o in order:
        j = turn(x, o)
        swaps[o].wait_recv()
        both = mm(pair[0, j, V:, :], pair[1, j, V:, :])
        if o == 0:
            row[x, V:, :] = both
        else:
            chip[o, V:, :] = both
            sends[o, 4] = along_x(o, tail, 4)
    for o in order:
        j = turn(x, o)
        swaps[4 + o].wait_recv()
        both = mm(pair[0, j, :V, :], pair[1, j, V:, :]) + pair[1, j, :V, :]
        if o == 0:
            row[x, :V, :] = both
        else:
            chip[o, :V, :] = both
            sends[o, 2] = along_x(o, quarter(2), 2)
    for part in (1, 3, 0):
        for o in (2, 1, 3):
            sends[o, part] = along_x(o, quarter(part), part)

    loads[4].wait()
    qf[...] = q_in[...].astype(F32).reshape(T * H, K)
    for h in heads:
        query = qf[pl.ds(h, T, stride=H), :]
        key_h = kf[pl.ds(h, T, stride=H), :].astype(BF16)
        rq = 1.0 / jnp.sqrt(jnp.sum(query * query, axis=1, keepdims=True) + 1e-06)
        seen = jnp.where(
            lower_incl, dot_nt(query.astype(BF16), key_h) * rq * rk_row[h], 0.0
        )
        gap = jnp.where(lower_incl, cum_col[h] - cum_row[h], 0.0)
        eff[h] = jnp.exp(cum_col[h]) * (query * rq - mm_nt(seen, w_all[h]))
        own[h] = mm_nt(seen * jnp.exp(gap), u_all[h])

    for o in (1, 3, 2):
        sends[o, 4].wait_recv()
    row_t = [row[k, V:, :] for k in range(4)]
    row_t10 = mm(row_t[0], row_t[1])
    row_t32 = mm(row_t[2], row_t[3])
    row_10[V:, :] = row_t10
    row_all[...] = mm(row_t10, row_t32)
    gives = {}
    for o in (2, 1, 3):
        gives[o] = copy(
            row_all, y_buf.at[y, pl.ds(Q, K)], ya_sem, o, {"seq_0": turn(y, o)}
        )
        gives[o].start()
        started.append(gives[o])
    y_buf[y, Q:, :] = row_all[...]
    weights_1 = weights(row_t[1])
    weights_3 = weights(row_t[3])
    weights_32 = weights(row_t32)
    for part in (2, 1, 3, 0):
        rows = quarter(part)
        for o in (1, 3, 2):
            sends[o, part].wait_recv()
        part_10 = fold(dot(side(row[0, rows, :]), weights_1)) + row[1, rows, :]
        part_32 = fold(dot(side(row[2, rows, :]), weights_3)) + row[3, rows, :]
        row_10[rows, :] = part_10
        total = fold(dot(side(part_10), weights_32)) + part_32
        if part == 0:
            y_buf[y, :Q, :] = total
        else:
            y_send[part] = total
            gives[4 + part] = copy(
                y_send.at[part],
                y_buf.at[y, pl.ds(0, Q)],
                ya_sem,
                4 + part,
                {"seq_0": turn(y, part)},
            )
            gives[4 + part].start()
            started.append(gives[4 + part])
    for o in (1, 3, 2):
        gives[o].wait_recv()
    plane_t = [y_buf[k, Q:, :] for k in range(4)]
    plane_t10 = mm(plane_t[0], plane_t[1])
    plane_t32 = mm(plane_t[2], plane_t[3])
    trans = mm(plane_t10, plane_t32)

    even = lax.rem(z, 2) == 0
    next_one = {"grp": lax.rem(z + 1, planes)}
    size = Q // PIECES
    pieces = [pl.ds(i * size, size) for i in range(PIECES)]
    two_on = {"grp": lax.rem(z + 2, planes)}
    give_trans = copy(
        p_send.at[pl.ds(Q, K)], p_buf.at[pl.ds(Q, K)], p_sem, PIECES, next_one
    )
    give_state, jump, step = [], [], []
    for i, rows in enumerate(pieces):
        give_state.append(copy(p_send.at[rows], p_buf.at[rows], p_sem, i, next_one))
        jump.append(copy(z_out.at[rows], z_in.at[rows], z_sem, i, two_on))
        step.append(copy(z_out.at[rows], z_in.at[rows], z_sem, PIECES + i, next_one))
    far = {}
    for o in (3, 4):
        there = {"grp": lax.rem(z + o, planes)}
        far[o] = [
            copy(z_out.at[rows], z_in.at[rows], z_sem, (o - 1) * PIECES + i, there)
            for i, rows in enumerate(pieces)
        ]
    hand = {1: copy(h_send, h_buf, h_sem, 0, next_one)}
    hand[2] = copy(h_send, h_buf, h_sem, 1, two_on)

    @pl.when(even & (z > 0))
    def _():
        p_send[Q:, :] = trans
        give_trans.start()

    for o in (3, 1, 2):
        gives[4 + o].wait_recv()
    plane_s = [y_buf[k, :Q, :] for k in range(4)]
    plane_s10 = mm(plane_s[0], plane_t[1]) + plane_s[1]
    plane_s32 = mm(plane_s[2], plane_t[3]) + plane_s[3]
    total = mm(plane_s10, plane_t32) + plane_s32

    @pl.when(even)
    def _():
        p_send[:Q, :] = total
        for part in give_state:
            part.start()

    row_210[...] = joined(row_10[...], row[2])
    plane_10 = jnp.concatenate([plane_s10, plane_t10], axis=0)
    plane_210 = joined(plane_10, y_buf[2])

    @pl.when(z == 0)
    def _():
        enter[...] = jnp.zeros_like(enter)

    @pl.when(z == 1)
    def _():
        for i, rows in enumerate(pieces):
            give_state[i].wait_recv()
            z_out[rows, :] = mm(p_buf[rows, :], trans) + total[i * size : (i + 1) * size]
            jump[i].start()
        for part in step:
            part.start()
        enter[...] = p_buf[:Q, :]

    @pl.when(z == 3)
    def _():
        give_trans.wait_recv()
        two_t = mm(p_buf[Q:, :], trans)
        for part in give_state:
            part.wait_recv()
        two_s = mm(p_buf[:Q, :], trans) + total
        for i, rows in enumerate(pieces):
            jump[i].wait_recv()
            z_out[rows, :] = mm(z_in[rows, :], two_t) + two_s[i * size : (i + 1) * size]
            far[4][i].start()
        for part in far[3] + jump + step:
            part.start()
        enter[...] = entered(z_in[...], p_buf[...])

    @pl.when(z == 5)
    def _():
        give_trans.wait_recv()
        h_send[Q:, :] = mm(p_buf[Q:, :], trans)
        for part in give_state:
            part.wait_recv()
        h_send[:Q, :] = mm(p_buf[:Q, :], trans) + total
        hand[2].start()
        hand[1].start()
        for part in jump:
            part.wait_recv()
        enter[...] = entered(z_in[...], p_buf[...])

    @pl.when(z == 6)
    def _():
        hand[1].wait_recv()
        for part in far[3]:
            part.wait_recv()
        enter[...] = entered(z_in[...], h_buf[...])

    @pl.when(z == 7)
    def _():
        give_trans.wait_recv()
        for part in give_state:
            part.wait_recv()
        hand[2].wait_recv()
        three = joined(h_buf[...], p_buf[...])
        for part in far[4]:
            part.wait_recv()
        enter[...] = entered(z_in[...], three)

    @pl.when((z == 2) | (z == 4))
    def _():
        for part in step:
            part.wait_recv()
        enter[...] = z_in[...]

    state = enter[...]
    r_send[0] = state
    r_send[1] = entered(state, y_buf[0])
    r_send[2] = entered(state, plane_10)
    r_send[3] = entered(state, plane_210)
    mine = pl.ds(pl.multiple_of(y * Q, Q), Q)
    sends = {}
    for o in (2, 1, 3):
        to = turn(y, o)
        sends[o] = copy(r_send.at[to], r_buf.at[mine], yb_sem, o, {"seq_0": to})
        sends[o].start()
        started.append(sends[o])
    r_buf[mine, :] = r_send[y]
    arrivals = {1: [], 2: [], 3: []}
    for o in (0, 1, 3, 2):
        if o > 0:
            sends[o].wait_recv()
        part = pl.ds(pl.multiple_of(turn(y, -o) * Q, Q), Q)
        state = r_buf[part, :]
        x_send[0, part, :] = state
        x_send[1, part, :] = mm(state, row[0, V:, :]) + row[0, part, :]
        x_send[2, part, :] = mm(state, row_10[V:, :]) + row_10[part, :]
        x_send[3, part, :] = mm(state, row_210[V:, :]) + row_210[part, :]
        for a in (2, 1, 3):
            to = turn(x, a)
            sent = copy(
                x_send.at[to, part], x_buf.at[x, part], xb_sem, 4 * a + o, {"seq_1": to}
            )
            sent.start()
            started.append(sent)
            arrivals[a].append(sent)
        x_buf[x, part, :] = x_send[x, part, :]

    def read_out(head):
        both = own[head] + mm_nt(eff[head], full[head])
        vf0[pl.ds(head, T, stride=H), :] = both[:, :K]
        vf1[pl.ds(head, T, stride=H), :] = both[:, K:]

    swaps = []
    for a in (0, 1, 3, 2):
        j = turn(x, -a)
        if a > 0:
            for sent in arrivals[a]:
                sent.wait_recv()
        first = x_buf[j]
        second = entered(first, pair[0, j])
        head = HH * c + j
        full[head] = jnp.where(c == 0, first, second)
        c_send[a] = jnp.where(c == 0, second, first)
        swap = copy(c_send.at[a], full.at[head], back_sem, a, {"seq_2": 1 - c})
        swap.start()
        started.append(swap)
        swaps.append((swap, j))
        read_out(head)
    for swap, j in swaps:
        swap.wait_recv()
        read_out(HH * (1 - c) + j)
    o_ref[:, :, :K] = vf0[...].reshape(T, H, K).astype(BF16)
    o_ref[:, :, K:] = vf1[...].reshape(T, H, K).astype(BF16)

    for sent in started:
        sent.wait_send()

    @pl.when(even)
    def _():
        for part in give_state:
            part.wait_send()

    @pl.when(even & (z > 0))
    def _():
        give_trans.wait_send()

    @pl.when((z == 1) | (z == 3))
    def _():
        for part in jump + step:
            part.wait_send()

    @pl.when(z == 3)
    def _():
        for part in far[3] + far[4]:
            part.wait_send()

    @pl.when(z == 5)
    def _():
        hand[1].wait_send()
        hand[2].wait_send()


def body(*given):
    queries, key_rows, value_rows, log_gate, beta_rate = [pltpu.with_memory_space_constraint(a, pltpu.HBM) for a in given]
    dma = pltpu.SemaphoreType.DMA

    def room(*shape):
        return pltpu.VMEM(shape, F32)

    return pl.pallas_call(
        scan_kernel,
        out_shape=jax.ShapeDtypeStruct((T, H, V), BF16),
        in_specs=[pl.BlockSpec(memory_space=pltpu.HBM)] * 5,
        out_specs=pl.BlockSpec(memory_space=pltpu.VMEM),
        scratch_shapes=[
            pltpu.VMEM((T, H, K), BF16),
            pltpu.VMEM((T, H, K), BF16),
            pltpu.VMEM((T, H, V), BF16),
            room(H, T),
            room(H, T),
            room(T * H, K),
            room(T * H, K),
            room(T * H, K),
            room(T * H, K),
            room(H, K, T),
            room(H, V, T),
            room(H, T, K),
            room(H, T, V),
            room(H, ROWS, K),
            room(2, HH, ROWS, K),
            room(4, ROWS, K),
            room(4, ROWS, K),
            room(ROWS, K),
            room(ROWS, K),
            room(K, K),
            room(4, Q, K),
            room(4, Q + K, K),
            room(Q + K, K),
            room(Q + K, K),
            room(Q + K, K),
            room(Q + K, K),
            room(Q, K),
            room(Q, K),
            room(Q, K),
            room(4, Q, K),
            room(V, K),
            room(4, V, K),
            room(4, V, K),
            room(4, V, K),
            room(H, V, K),
            dma((5,)),
            dma((2, 8)),
            dma((2, 15)),
            dma((2, 8)),
            dma((2, PIECES + 1)),
            dma((2, 2)),
            dma((2, 4 * PIECES)),
            dma((2, 4)),
            dma((2, 16)),
            dma((2, 4)),
        ],
        compiler_params=pltpu.CompilerParams(
            collective_id=0, has_side_effects=True, vmem_limit_bytes=48 * 1024 * 1024
        ),
        name="scan",
    )(queries, key_rows, value_rows, log_gate, beta_rate)


def solution(mesh):
    finer = Mesh(
        mesh.devices.reshape(4, 4, 2, mesh.shape["grp"]), ("seq_0", "seq_1", "seq_2", "grp")
    )
    placed = (
        P(GRP_SEQ, None, None),
        P(GRP_SEQ, None, None),
        P(GRP_SEQ, None, None),
        P(None, GRP_SEQ),
        P(None, GRP_SEQ),
    )
    return jax.shard_map(
        body, mesh=finer, in_specs=placed, out_specs=P(GRP_SEQ, None, None), check_vma=False
    )
```

```python
import functools

import jax
import jax.numpy as jnp
from jax import lax
from jax.experimental import pallas as pl
from jax.experimental.pallas import tpu as pltpu
from jax.sharding import Mesh
from jax.sharding import PartitionSpec as P

GRP_SEQ = ("grp", "seq_0", "seq_1", "seq_2")
MESH = pl.DeviceIdType.MESH
F32 = jnp.float32
BF16 = jnp.bfloat16

T = 128
K = 128
V = 256
H = 8
HH = 4
Q = 64
NEAR = 16
LINKED = (
    (0, 1),
    (1, 2),
    (1, 3),
    (2, 3),
    (3, 4),
    (3, 5),
    (3, 6),
    (3, 7),
    (4, 5),
    (5, 6),
    (5, 7),
    (6, 7),
)
PIECES = 2
ROWS = V + K


def dot(a, b):
    return lax.dot_general(a, b, (((1,), (0,)), ((), ())), preferred_element_type=F32)


def dot_nt(a, b):
    return lax.dot_general(a, b, (((1,), (1,)), ((), ())), preferred_element_type=F32)


def split(x):
    high = x.astype(BF16)
    low = (x - high.astype(F32)).astype(BF16)
    return high, low


def side(x):
    return jnp.concatenate(split(x), axis=1)


def fold(wide):
    half = wide.shape[1] // 2
    return wide[:, :half] + wide[:, half:]


def weights(w):
    pair = side(w)
    return jnp.concatenate([pair, pair], axis=0)


def mm(x, w):
    count = x.shape[0]
    if count > Q:
        return fold(dot(side(x), weights(w)))
    both = fold(dot(jnp.concatenate(split(x), axis=0), side(w)))
    return both[:count] + both[count:]


def mm_nt(x, y):
    wide = side(x)
    high, low = split(y)
    return dot_nt(wide, jnp.concatenate([high, high], axis=1)) + dot_nt(
        wide, jnp.concatenate([low, low], axis=1)
    )


def joined(earlier, later):
    top = later.shape[0] - K
    moved = mm(earlier, later[top:])
    return jnp.concatenate([moved[:top] + later[:top], moved[top:]], axis=0)


def entered(state, before):
    top = before.shape[0] - K
    return mm(state, before[top:]) + before[:top]


def turn(at, o):
    return lax.rem(at + o + 4, 4)


def scan_kernel(
    q_ref,
    k_ref,
    v_ref,
    lg_ref,
    be_ref,
    o_ref,
    q_in,
    k_in,
    v_in,
    lg_in,
    be_in,
    qf,
    kf,
    vf0,
    vf1,
    w_all,
    u_all,
    eff,
    own,
    maps,
    pair,
    chip,
    row,
    row_10,
    row_210,
    row_all,
    y_send,
    y_buf,
    p_send,
    p_buf,
    h_send,
    h_buf,
    z_in,
    z_out,
    enter,
    r_send,
    r_buf,
    x_send,
    x_buf,
    c_send,
    full,
    in_sem,
    core_sem,
    xa_sem,
    ya_sem,
    p_sem,
    h_sem,
    z_sem,
    yb_sem,
    xb_sem,
    back_sem,
):
    y = lax.axis_index("seq_0")
    x = lax.axis_index("seq_1")
    c = lax.axis_index("seq_2")
    z = lax.axis_index("grp")
    planes = lax.axis_size("grp")
    heads = range(H)

    loads = []
    for i, (src, dst) in enumerate(
        ((k_ref, k_in), (lg_ref, lg_in), (be_ref, be_in), (v_ref, v_in), (q_ref, q_in))
    ):
        loads.append(pltpu.make_async_copy(src, dst, in_sem.at[i]))
        loads[i].start()

    barrier = pltpu.get_barrier_semaphore()
    peers = [{"seq_2": 1 - c}]
    peers += [{"seq_1": turn(x, o)} for o in (1, 2, 3)]
    peers += [{"seq_0": turn(y, o)} for o in (1, 2, 3)]
    for peer in peers:
        pl.semaphore_signal(barrier, inc=1, device_id=peer, device_id_type=MESH)
    greeted = jnp.int32(len(peers))
    for low, high in LINKED:
        for at, o in ((low, high - low), (high, low - high)):
            greeted = greeted + jnp.where(z == at, 1, 0)

            @pl.when(z == at)
            def _():
                there = {"grp": lax.rem(z + planes + o, planes)}
                pl.semaphore_signal(barrier, inc=1, device_id=there, device_id_type=MESH)


    def copy(src, dst, sem, o, peer):
        return pltpu.make_async_remote_copy(
            src_ref=src,
            dst_ref=dst,
            send_sem=sem.at[0, o],
            recv_sem=sem.at[1, o],
            device_id=peer,
            device_id_type=MESH,
        )

    started = []

    rows_idx = lax.broadcasted_iota(jnp.int32, (T, T), 0)
    cols_idx = lax.broadcasted_iota(jnp.int32, (T, T), 1)
    differ = rows_idx ^ cols_idx
    upper = rows_idx < cols_idx
    upper_incl = rows_idx <= cols_idx
    lower_incl = rows_idx >= cols_idx
    eye = (rows_idx == cols_idx).astype(F32)
    loads[0].wait()
    kf[...] = k_in[...].astype(F32).reshape(T * H, K)
    key = [kf[pl.ds(h, T, stride=H), :] for h in heads]
    key_b = [key[h].astype(BF16) for h in heads]
    key_t = [key[h].T for h in heads]
    squares = jnp.concatenate(
        [jnp.sum(key_t[h] * key_t[h], axis=0, keepdims=True) for h in heads], axis=0
    )
    key_tb = [key_t[h].astype(BF16) for h in heads]
    loads[1].wait()
    loads[2].wait()
    beta = be_in[...]
    cum = jnp.dot(
        lg_in[...],
        upper_incl.astype(F32),
        precision=lax.Precision.HIGHEST,
        preferred_element_type=F32,
    )
    rk = 1.0 / jnp.sqrt(squares + 1e-06)
    columns = jnp.concatenate([rk, beta, cum, jnp.zeros((T - 3 * H, T), F32)], axis=0).T
    rk_col = [columns[:, h : h + 1] for h in heads]
    be_col = [columns[:, H + h : H + h + 1] for h in heads]
    cum_col = [columns[:, 2 * H + h : 2 * H + h + 1] for h in heads]
    rk_row = [rk[h : h + 1, :] for h in heads]
    be_row = [beta[h : h + 1, :] for h in heads]
    cum_row = [cum[h : h + 1, :] for h in heads]
    strict = [
        jnp.where(
            upper, dot_nt(key_b[h], key_b[h]) * rk_col[h] * (be_row[h] * rk_row[h]), 0.0
        )
        for h in heads
    ]
    near = [jnp.where(differ < NEAR, strict[h], 0.0) for h in heads]
    inverse = [eye - near[h] for h in heads]
    power = [mm(near[h], near[h]) for h in heads]
    reach = 4
    while reach < NEAR:
        grown = [
            mm(jnp.concatenate([inverse[h], power[h]], axis=0), power[h]) for h in heads
        ]
        inverse = [inverse[h] + grown[h][:T] for h in heads]
        power = [grown[h][T:] for h in heads]
        reach = reach * 2
    inverse = [inverse[h] + mm(inverse[h], power[h]) for h in heads]
    span = NEAR
    while span < T:
        level = (differ >= span) & (differ < 2 * span)
        starts = range(0, T, 2 * span)
        left = [
            mm(
                jnp.concatenate([inverse[h][a : a + span] for a in starts], axis=0),
                jnp.where(level, strict[h], 0.0),
            )
            for h in heads
        ]
        change = [mm(left[h], inverse[h]) for h in heads]
        inverse = [
            jnp.concatenate(
                [
                    piece
                    for i, a in enumerate(starts)
                    for piece in (
                        inverse[h][a : a + span] - change[h][i * span : (i + 1) * span],
                        inverse[h][a + span : a + 2 * span],
                    )
                ],
                axis=0,
            )
            for h in heads
        ]
        span = span * 2
    twice = [jnp.concatenate([key_b[h], key_b[h]], axis=0) for h in heads]
    last = [cum[h : h + 1, T - 1 : T] for h in heads]
    for h in heads:
        w_t = fold(dot(key_tb[h], side(inverse[h] * (be_col[h] * rk_col[h]))))
        moved = dot(side(w_t * (rk_row[h] * -jnp.exp(last[h]))), twice[h])
        maps[h, V:, :] = moved + eye * jnp.exp(last[h])
        w_all[h] = w_t

    pl.semaphore_wait(barrier, greeted)

    order = (2, 1, 3, 0)
    tail = pl.ds(V, K)
    body_rows = pl.ds(0, V)
    swaps = {}

    def swap_cores(i, o, rows):
        j = turn(x, o)
        swaps[i + o] = copy(
            maps.at[HH * (1 - c) + j, rows],
            pair.at[c, j, rows],
            core_sem,
            i + o,
            {"seq_2": 1 - c},
        )
        swaps[i + o].start()
        started.append(swaps[i + o])

    for o in order:
        swap_cores(0, o, tail)
    loads[3].wait()
    vf0[...] = v_in[:, :, :K].astype(F32).reshape(T * H, K)
    vf1[...] = v_in[:, :, K:].astype(F32).reshape(T * H, K)
    for h in heads:
        gap = jnp.where(upper_incl, cum_row[h] - cum_col[h], 0.0)
        decay_t = jnp.where(upper_incl, jnp.exp(gap), 0.0)
        value_t = jnp.concatenate(
            [vf0[pl.ds(h, T, stride=H), :].T, vf1[pl.ds(h, T, stride=H), :].T], axis=0
        ).astype(BF16)
        u_t = fold(dot(value_t, side(inverse[h] * decay_t * be_col[h])))
        scaled = u_t * (rk_row[h] * jnp.exp(last[h] - cum_row[h]))
        maps[h, :V, :] = dot(side(scaled), twice[h])
        u_all[h] = u_t
    for o in order:
        swap_cores(4, o, body_rows)
    for o in order:
        j = turn(x, o)
        pair[c, j] = maps[HH * c + j]

    def along_x(o, rows, slot):
        sent = copy(
            chip.at[o, rows],
            row.at[x, rows],
            xa_sem,
            5 * (o - 1) + slot,
            {"seq_1": turn(x, o)},
        )
        sent.start()
        started.append(sent)
        return sent

    def quarter(o):
        return pl.ds(pl.multiple_of(turn(y, o) * Q, Q), Q)

    sends = {}
    for o in order:
        j = turn(x, o)
        swaps[o].wait_recv()
        both = mm(pair[0, j, V:, :], pair[1, j, V:, :])
        if o == 0:
            row[x, V:, :] = both
        else:
            chip[o, V:, :] = both
            sends[o, 4] = along_x(o, tail, 4)
    for o in order:
        j = turn(x, o)
        swaps[4 + o].wait_recv()
        both = mm(pair[0, j, :V, :], pair[1, j, V:, :]) + pair[1, j, :V, :]
        if o == 0:
            row[x, :V, :] = both
        else:
            chip[o, :V, :] = both
            sends[o, 2] = along_x(o, quarter(2), 2)
    for part in (1, 3, 0):
        for o in (2, 1, 3):
            sends[o, part] = along_x(o, quarter(part), part)

    loads[4].wait()
    qf[...] = q_in[...].astype(F32).reshape(T * H, K)
    for h in heads:
        query = qf[pl.ds(h, T, stride=H), :]
        key_h = kf[pl.ds(h, T, stride=H), :].astype(BF16)
        rq = 1.0 / jnp.sqrt(jnp.sum(query * query, axis=1, keepdims=True) + 1e-06)
        seen = jnp.where(
            lower_incl, dot_nt(query.astype(BF16), key_h) * rq * rk_row[h], 0.0
        )
        gap = jnp.where(lower_incl, cum_col[h] - cum_row[h], 0.0)
        eff[h] = jnp.exp(cum_col[h]) * (query * rq - mm_nt(seen, w_all[h]))
        own[h] = mm_nt(seen * jnp.exp(gap), u_all[h])

    for o in (1, 3, 2):
        sends[o, 4].wait_recv()
    row_t = [row[k, V:, :] for k in range(4)]
    row_t10 = mm(row_t[0], row_t[1])
    row_t32 = mm(row_t[2], row_t[3])
    row_10[V:, :] = row_t10
    row_all[...] = mm(row_t10, row_t32)
    gives = {}
    for o in (2, 1, 3):
        gives[o] = copy(
            row_all, y_buf.at[y, pl.ds(Q, K)], ya_sem, o, {"seq_0": turn(y, o)}
        )
        gives[o].start()
        started.append(gives[o])
    y_buf[y, Q:, :] = row_all[...]
    weights_1 = weights(row_t[1])
    weights_3 = weights(row_t[3])
    weights_32 = weights(row_t32)
    for part in (2, 1, 3, 0):
        rows = quarter(part)
        for o in (1, 3, 2):
            sends[o, part].wait_recv()
        part_10 = fold(dot(side(row[0, rows, :]), weights_1)) + row[1, rows, :]
        part_32 = fold(dot(side(row[2, rows, :]), weights_3)) + row[3, rows, :]
        row_10[rows, :] = part_10
        total = fold(dot(side(part_10), weights_32)) + part_32
        if part == 0:
            y_buf[y, :Q, :] = total
        else:
            y_send[part] = total
            gives[4 + part] = copy(
                y_send.at[part],
                y_buf.at[y, pl.ds(0, Q)],
                ya_sem,
                4 + part,
                {"seq_0": turn(y, part)},
            )
            gives[4 + part].start()
            started.append(gives[4 + part])
    for o in (1, 3, 2):
        gives[o].wait_recv()
    plane_t = [y_buf[k, Q:, :] for k in range(4)]
    plane_t10 = mm(plane_t[0], plane_t[1])
    plane_t32 = mm(plane_t[2], plane_t[3])
    trans = mm(plane_t10, plane_t32)

    even = lax.rem(z, 2) == 0
    next_one = {"grp": lax.rem(z + 1, planes)}
    size = Q // PIECES
    pieces = [pl.ds(i * size, size) for i in range(PIECES)]
    two_on = {"grp": lax.rem(z + 2, planes)}
    give_trans = copy(
        p_send.at[pl.ds(Q, K)], p_buf.at[pl.ds(Q, K)], p_sem, PIECES, next_one
    )
    give_state, jump, step = [], [], []
    for i, rows in enumerate(pieces):
        give_state.append(copy(p_send.at[rows], p_buf.at[rows], p_sem, i, next_one))
        jump.append(copy(z_out.at[rows], z_in.at[rows], z_sem, i, two_on))
        step.append(copy(z_out.at[rows], z_in.at[rows], z_sem, PIECES + i, next_one))
    far = {}
    for o in (3, 4):
        there = {"grp": lax.rem(z + o, planes)}
        far[o] = [
            copy(z_out.at[rows], z_in.at[rows], z_sem, (o - 1) * PIECES + i, there)
            for i, rows in enumerate(pieces)
        ]
    hand = {1: copy(h_send, h_buf, h_sem, 0, next_one)}
    hand[2] = copy(h_send, h_buf, h_sem, 1, two_on)

    @pl.when(even & (z > 0))
    def _():
        p_send[Q:, :] = trans
        give_trans.start()

    for o in (3, 1, 2):
        gives[4 + o].wait_recv()
    plane_s = [y_buf[k, :Q, :] for k in range(4)]
    plane_s10 = mm(plane_s[0], plane_t[1]) + plane_s[1]
    plane_s32 = mm(plane_s[2], plane_t[3]) + plane_s[3]
    total = mm(plane_s10, plane_t32) + plane_s32

    @pl.when(even)
    def _():
        p_send[:Q, :] = total
        for part in give_state:
            part.start()

    row_210[...] = joined(row_10[...], row[2])
    plane_10 = jnp.concatenate([plane_s10, plane_t10], axis=0)
    plane_210 = joined(plane_10, y_buf[2])

    @pl.when(z == 0)
    def _():
        enter[...] = jnp.zeros_like(enter)

    @pl.when(z == 1)
    def _():
        for i, rows in enumerate(pieces):
            give_state[i].wait_recv()
            z_out[rows, :] = mm(p_buf[rows, :], trans) + total[i * size : (i + 1) * size]
            jump[i].start()
        for part in step:
            part.start()
        enter[...] = p_buf[:Q, :]

    @pl.when(z == 3)
    def _():
        give_trans.wait_recv()
        two_t = mm(p_buf[Q:, :], trans)
        for part in give_state:
            part.wait_recv()
        two_s = mm(p_buf[:Q, :], trans) + total
        for i, rows in enumerate(pieces):
            jump[i].wait_recv()
            z_out[rows, :] = mm(z_in[rows, :], two_t) + two_s[i * size : (i + 1) * size]
            far[4][i].start()
        for part in far[3] + jump + step:
            part.start()
        enter[...] = entered(z_in[...], p_buf[...])

    @pl.when(z == 5)
    def _():
        give_trans.wait_recv()
        h_send[Q:, :] = mm(p_buf[Q:, :], trans)
        for part in give_state:
            part.wait_recv()
        h_send[:Q, :] = mm(p_buf[:Q, :], trans) + total
        hand[2].start()
        hand[1].start()
        for part in jump:
            part.wait_recv()
        enter[...] = entered(z_in[...], p_buf[...])

    @pl.when(z == 6)
    def _():
        hand[1].wait_recv()
        for part in far[3]:
            part.wait_recv()
        enter[...] = entered(z_in[...], h_buf[...])

    @pl.when(z == 7)
    def _():
        give_trans.wait_recv()
        for part in give_state:
            part.wait_recv()
        hand[2].wait_recv()
        three = joined(h_buf[...], p_buf[...])
        for part in far[4]:
            part.wait_recv()
        enter[...] = entered(z_in[...], three)

    @pl.when((z == 2) | (z == 4))
    def _():
        for part in step:
            part.wait_recv()
        enter[...] = z_in[...]

    state = enter[...]
    r_send[0] = state
    r_send[1] = entered(state, y_buf[0])
    r_send[2] = entered(state, plane_10)
    r_send[3] = entered(state, plane_210)
    mine = pl.ds(pl.multiple_of(y * Q, Q), Q)
    sends = {}
    for o in (2, 1, 3):
        to = turn(y, o)
        sends[o] = copy(r_send.at[to], r_buf.at[mine], yb_sem, o, {"seq_0": to})
        sends[o].start()
        started.append(sends[o])
    r_buf[mine, :] = r_send[y]
    arrivals = {1: [], 2: [], 3: []}
    for o in (0, 1, 3, 2):
        if o > 0:
            sends[o].wait_recv()
        part = pl.ds(pl.multiple_of(turn(y, -o) * Q, Q), Q)
        state = r_buf[part, :]
        x_send[0, part, :] = state
        x_send[1, part, :] = mm(state, row[0, V:, :]) + row[0, part, :]
        x_send[2, part, :] = mm(state, row_10[V:, :]) + row_10[part, :]
        x_send[3, part, :] = mm(state, row_210[V:, :]) + row_210[part, :]
        for a in (2, 1, 3):
            to = turn(x, a)
            sent = copy(
                x_send.at[to, part], x_buf.at[x, part], xb_sem, 4 * a + o, {"seq_1": to}
            )
            sent.start()
            started.append(sent)
            arrivals[a].append(sent)
        x_buf[x, part, :] = x_send[x, part, :]

    def read_out(head):
        both = own[head] + mm_nt(eff[head], full[head])
        vf0[pl.ds(head, T, stride=H), :] = both[:, :K]
        vf1[pl.ds(head, T, stride=H), :] = both[:, K:]

    swaps = []
    for a in (0, 1, 3, 2):
        j = turn(x, -a)
        if a > 0:
            for sent in arrivals[a]:
                sent.wait_recv()
        first = x_buf[j]
        second = entered(first, pair[0, j])
        head = HH * c + j
        full[head] = jnp.where(c == 0, first, second)
        c_send[a] = jnp.where(c == 0, second, first)
        swap = copy(c_send.at[a], full.at[head], back_sem, a, {"seq_2": 1 - c})
        swap.start()
        started.append(swap)
        swaps.append((swap, j))
        read_out(head)
    for swap, j in swaps:
        swap.wait_recv()
        read_out(HH * (1 - c) + j)
    o_ref[:, :, :K] = vf0[...].reshape(T, H, K).astype(BF16)
    o_ref[:, :, K:] = vf1[...].reshape(T, H, K).astype(BF16)

    for sent in started:
        sent.wait_send()

    @pl.when(even)
    def _():
        for part in give_state:
            part.wait_send()

    @pl.when(even & (z > 0))
    def _():
        give_trans.wait_send()

    @pl.when((z == 1) | (z == 3))
    def _():
        for part in jump + step:
            part.wait_send()

    @pl.when(z == 3)
    def _():
        for part in far[3] + far[4]:
            part.wait_send()

    @pl.when(z == 5)
    def _():
        hand[1].wait_send()
        hand[2].wait_send()


def body(*given):
    queries, key_rows, value_rows, log_gate, beta_rate = [pltpu.with_memory_space_constraint(a, pltpu.HBM) for a in given]
    dma = pltpu.SemaphoreType.DMA

    def room(*shape):
        return pltpu.VMEM(shape, F32)

    return pl.pallas_call(
        scan_kernel,
        out_shape=jax.ShapeDtypeStruct((T, H, V), BF16),
        in_specs=[pl.BlockSpec(memory_space=pltpu.HBM)] * 5,
        out_specs=pl.BlockSpec(memory_space=pltpu.VMEM),
        scratch_shapes=[
            pltpu.VMEM((T, H, K), BF16),
            pltpu.VMEM((T, H, K), BF16),
            pltpu.VMEM((T, H, V), BF16),
            room(H, T),
            room(H, T),
            room(T * H, K),
            room(T * H, K),
            room(T * H, K),
            room(T * H, K),
            room(H, K, T),
            room(H, V, T),
            room(H, T, K),
            room(H, T, V),
            room(H, ROWS, K),
            room(2, HH, ROWS, K),
            room(4, ROWS, K),
            room(4, ROWS, K),
            room(ROWS, K),
            room(ROWS, K),
            room(K, K),
            room(4, Q, K),
            room(4, Q + K, K),
            room(Q + K, K),
            room(Q + K, K),
            room(Q + K, K),
            room(Q + K, K),
            room(Q, K),
            room(Q, K),
            room(Q, K),
            room(4, Q, K),
            room(V, K),
            room(4, V, K),
            room(4, V, K),
            room(4, V, K),
            room(H, V, K),
            dma((5,)),
            dma((2, 8)),
            dma((2, 15)),
            dma((2, 8)),
            dma((2, PIECES + 1)),
            dma((2, 2)),
            dma((2, 4 * PIECES)),
            dma((2, 4)),
            dma((2, 16)),
            dma((2, 4)),
        ],
        compiler_params=pltpu.CompilerParams(
            collective_id=0, has_side_effects=True, vmem_limit_bytes=48 * 1024 * 1024
        ),
        name="scan",
    )(queries, key_rows, value_rows, log_gate, beta_rate)


def solution(mesh):
    finer = Mesh(
        mesh.devices.reshape(4, 4, 2, mesh.shape["grp"]), ("seq_0", "seq_1", "seq_2", "grp")
    )
    placed = (
        P(GRP_SEQ, None, None),
        P(GRP_SEQ, None, None),
        P(GRP_SEQ, None, None),
        P(None, GRP_SEQ),
        P(None, GRP_SEQ),
    )
    return jax.shard_map(
        body, mesh=finer, in_specs=placed, out_specs=P(GRP_SEQ, None, None), check_vma=False
    )
```

```python
import functools

import jax
import jax.numpy as jnp
from jax import lax
from jax.experimental import pallas as pl
from jax.experimental.pallas import tpu as pltpu
from jax.sharding import Mesh
from jax.sharding import PartitionSpec as P

GRP_SEQ = ("grp", "seq_0", "seq_1", "seq_2")
MESH = pl.DeviceIdType.MESH
F32 = jnp.float32
BF16 = jnp.bfloat16

T = 128
K = 128
V = 256
H = 8
HH = 4
Q = 64
NEAR = 16
LINKED = (
    (0, 1),
    (1, 2),
    (1, 3),
    (2, 3),
    (3, 4),
    (3, 5),
    (3, 6),
    (3, 7),
    (4, 5),
    (5, 6),
    (5, 7),
    (6, 7),
)
PIECES = 2
ROWS = V + K


def dot(a, b):
    return lax.dot_general(a, b, (((1,), (0,)), ((), ())), preferred_element_type=F32)


def dot_nt(a, b):
    return lax.dot_general(a, b, (((1,), (1,)), ((), ())), preferred_element_type=F32)


def split(x):
    high = x.astype(BF16)
    low = (x - high.astype(F32)).astype(BF16)
    return high, low


def side(x):
    return jnp.concatenate(split(x), axis=1)


def fold(wide):
    half = wide.shape[1] // 2
    return wide[:, :half] + wide[:, half:]


def weights(w):
    pair = side(w)
    return jnp.concatenate([pair, pair], axis=0)


def mm(x, w):
    count = x.shape[0]
    if count > Q:
        return fold(dot(side(x), weights(w)))
    both = fold(dot(jnp.concatenate(split(x), axis=0), side(w)))
    return both[:count] + both[count:]


def through(x, sided):
    count = x.shape[0]
    both = fold(dot(jnp.concatenate(split(x), axis=0), sided))
    return both[:count] + both[count:]


def mm_nt(x, y):
    wide = side(x)
    high, low = split(y)
    return dot_nt(wide, jnp.concatenate([high, high], axis=1)) + dot_nt(
        wide, jnp.concatenate([low, low], axis=1)
    )


def joined(earlier, later):
    top = later.shape[0] - K
    moved = mm(earlier, later[top:])
    return jnp.concatenate([moved[:top] + later[:top], moved[top:]], axis=0)


def entered(state, before):
    top = before.shape[0] - K
    return mm(state, before[top:]) + before[:top]


def turn(at, o):
    return lax.rem(at + o + 4, 4)


def scan_kernel(
    q_ref,
    k_ref,
    v_ref,
    lg_ref,
    be_ref,
    o_ref,
    q_in,
    k_in,
    v_in,
    lg_in,
    be_in,
    qf,
    kf,
    vf0,
    vf1,
    w_all,
    u_all,
    eff,
    own,
    maps,
    pair,
    chip,
    row,
    row_10,
    row_210,
    row_all,
    y_send,
    y_buf,
    p_send,
    p_buf,
    h_send,
    h_buf,
    z_in,
    z_out,
    enter,
    r_send,
    r_buf,
    x_send,
    x_buf,
    c_send,
    full,
    in_sem,
    core_sem,
    xa_sem,
    ya_sem,
    p_sem,
    h_sem,
    z_sem,
    yb_sem,
    xb_sem,
    back_sem,
):
    y = lax.axis_index("seq_0")
    x = lax.axis_index("seq_1")
    c = lax.axis_index("seq_2")
    z = lax.axis_index("grp")
    planes = lax.axis_size("grp")
    heads = range(H)

    loads = []
    for i, (src, dst) in enumerate(
        ((k_ref, k_in), (lg_ref, lg_in), (be_ref, be_in), (v_ref, v_in), (q_ref, q_in))
    ):
        loads.append(pltpu.make_async_copy(src, dst, in_sem.at[i]))
        loads[i].start()

    barrier = pltpu.get_barrier_semaphore()
    peers = [{"seq_2": 1 - c}]
    peers += [{"seq_1": turn(x, o)} for o in (1, 2, 3)]
    peers += [{"seq_0": turn(y, o)} for o in (1, 2, 3)]
    for peer in peers:
        pl.semaphore_signal(barrier, inc=1, device_id=peer, device_id_type=MESH)
    greeted = jnp.int32(len(peers))
    for low, high in LINKED:
        for at, o in ((low, high - low), (high, low - high)):
            greeted = greeted + jnp.where(z == at, 1, 0)

            @pl.when(z == at)
            def _():
                there = {"grp": lax.rem(z + planes + o, planes)}
                pl.semaphore_signal(barrier, inc=1, device_id=there, device_id_type=MESH)


    def copy(src, dst, sem, o, peer):
        return pltpu.make_async_remote_copy(
            src_ref=src,
            dst_ref=dst,
            send_sem=sem.at[0, o],
            recv_sem=sem.at[1, o],
            device_id=peer,
            device_id_type=MESH,
        )

    started = []

    rows_idx = lax.broadcasted_iota(jnp.int32, (T, T), 0)
    cols_idx = lax.broadcasted_iota(jnp.int32, (T, T), 1)
    differ = rows_idx ^ cols_idx
    upper = rows_idx < cols_idx
    upper_incl = rows_idx <= cols_idx
    lower_incl = rows_idx >= cols_idx
    eye = (rows_idx == cols_idx).astype(F32)
    loads[0].wait()
    kf[...] = k_in[...].astype(F32).reshape(T * H, K)
    key = [kf[pl.ds(h, T, stride=H), :] for h in heads]
    key_b = [key[h].astype(BF16) for h in heads]
    key_t = [key[h].T for h in heads]
    squares = jnp.concatenate(
        [jnp.sum(key_t[h] * key_t[h], axis=0, keepdims=True) for h in heads], axis=0
    )
    key_tb = [key_t[h].astype(BF16) for h in heads]
    loads[1].wait()
    loads[2].wait()
    beta = be_in[...]
    cum = jnp.dot(
        lg_in[...],
        upper_incl.astype(F32),
        precision=lax.Precision.HIGHEST,
        preferred_element_type=F32,
    )
    rk = 1.0 / jnp.sqrt(squares + 1e-06)
    columns = jnp.concatenate([rk, beta, cum, jnp.zeros((T - 3 * H, T), F32)], axis=0).T
    rk_col = [columns[:, h : h + 1] for h in heads]
    be_col = [columns[:, H + h : H + h + 1] for h in heads]
    cum_col = [columns[:, 2 * H + h : 2 * H + h + 1] for h in heads]
    rk_row = [rk[h : h + 1, :] for h in heads]
    be_row = [beta[h : h + 1, :] for h in heads]
    cum_row = [cum[h : h + 1, :] for h in heads]
    strict = [
        jnp.where(
            upper, dot_nt(key_b[h], key_b[h]) * rk_col[h] * (be_row[h] * rk_row[h]), 0.0
        )
        for h in heads
    ]
    near = [jnp.where(differ < NEAR, strict[h], 0.0) for h in heads]
    inverse = [eye - near[h] for h in heads]
    power = [mm(near[h], near[h]) for h in heads]
    reach = 4
    while reach < NEAR:
        grown = [
            mm(jnp.concatenate([inverse[h], power[h]], axis=0), power[h]) for h in heads
        ]
        inverse = [inverse[h] + grown[h][:T] for h in heads]
        power = [grown[h][T:] for h in heads]
        reach = reach * 2
    inverse = [inverse[h] + mm(inverse[h], power[h]) for h in heads]
    span = NEAR
    while span < T:
        level = (differ >= span) & (differ < 2 * span)
        starts = range(0, T, 2 * span)
        left = [
            mm(
                jnp.concatenate([inverse[h][a : a + span] for a in starts], axis=0),
                jnp.where(level, strict[h], 0.0),
            )
            for h in heads
        ]
        change = [mm(left[h], inverse[h]) for h in heads]
        inverse = [
            jnp.concatenate(
                [
                    piece
                    for i, a in enumerate(starts)
                    for piece in (
                        inverse[h][a : a + span] - change[h][i * span : (i + 1) * span],
                        inverse[h][a + span : a + 2 * span],
                    )
                ],
                axis=0,
            )
            for h in heads
        ]
        span = span * 2
    twice = [jnp.concatenate([key_b[h], key_b[h]], axis=0) for h in heads]
    last = [cum[h : h + 1, T - 1 : T] for h in heads]
    for h in heads:
        w_t = fold(dot(key_tb[h], side(inverse[h] * (be_col[h] * rk_col[h]))))
        moved = dot(side(w_t * (rk_row[h] * -jnp.exp(last[h]))), twice[h])
        maps[h, V:, :] = moved + eye * jnp.exp(last[h])
        w_all[h] = w_t

    pl.semaphore_wait(barrier, greeted)

    order = (2, 1, 3, 0)
    tail = pl.ds(V, K)
    body_rows = pl.ds(0, V)
    swaps = {}

    def swap_cores(i, o, rows):
        j = turn(x, o)
        swaps[i + o] = copy(
            maps.at[HH * (1 - c) + j, rows],
            pair.at[c, j, rows],
            core_sem,
            i + o,
            {"seq_2": 1 - c},
        )
        swaps[i + o].start()
        started.append(swaps[i + o])

    for o in order:
        swap_cores(0, o, tail)
    loads[3].wait()
    vf0[...] = v_in[:, :, :K].astype(F32).reshape(T * H, K)
    vf1[...] = v_in[:, :, K:].astype(F32).reshape(T * H, K)
    for h in heads:
        gap = jnp.where(upper_incl, cum_row[h] - cum_col[h], 0.0)
        decay_t = jnp.where(upper_incl, jnp.exp(gap), 0.0)
        value_t = jnp.concatenate(
            [vf0[pl.ds(h, T, stride=H), :].T, vf1[pl.ds(h, T, stride=H), :].T], axis=0
        ).astype(BF16)
        u_t = fold(dot(value_t, side(inverse[h] * decay_t * be_col[h])))
        scaled = u_t * (rk_row[h] * jnp.exp(last[h] - cum_row[h]))
        maps[h, :V, :] = dot(side(scaled), twice[h])
        u_all[h] = u_t
    for o in order:
        swap_cores(4, o, body_rows)
    for o in order:
        j = turn(x, o)
        pair[c, j] = maps[HH * c + j]

    def along_x(o, rows, slot):
        sent = copy(
            chip.at[o, rows],
            row.at[x, rows],
            xa_sem,
            5 * (o - 1) + slot,
            {"seq_1": turn(x, o)},
        )
        sent.start()
        started.append(sent)
        return sent

    def quarter(o):
        return pl.ds(pl.multiple_of(turn(y, o) * Q, Q), Q)

    sends = {}
    for o in order:
        j = turn(x, o)
        swaps[o].wait_recv()
        both = mm(pair[0, j, V:, :], pair[1, j, V:, :])
        if o == 0:
            row[x, V:, :] = both
        else:
            chip[o, V:, :] = both
            sends[o, 4] = along_x(o, tail, 4)
    for o in order:
        j = turn(x, o)
        swaps[4 + o].wait_recv()
        both = mm(pair[0, j, :V, :], pair[1, j, V:, :]) + pair[1, j, :V, :]
        if o == 0:
            row[x, :V, :] = both
        else:
            chip[o, :V, :] = both
            sends[o, 2] = along_x(o, quarter(2), 2)
    for part in (1, 3, 0):
        for o in (2, 1, 3):
            sends[o, part] = along_x(o, quarter(part), part)

    loads[4].wait()
    qf[...] = q_in[...].astype(F32).reshape(T * H, K)
    for h in heads:
        query = qf[pl.ds(h, T, stride=H), :]
        key_h = kf[pl.ds(h, T, stride=H), :].astype(BF16)
        rq = 1.0 / jnp.sqrt(jnp.sum(query * query, axis=1, keepdims=True) + 1e-06)
        seen = jnp.where(
            lower_incl, dot_nt(query.astype(BF16), key_h) * rq * rk_row[h], 0.0
        )
        gap = jnp.where(lower_incl, cum_col[h] - cum_row[h], 0.0)
        eff[h] = jnp.exp(cum_col[h]) * (query * rq - mm_nt(seen, w_all[h]))
        own[h] = mm_nt(seen * jnp.exp(gap), u_all[h])

    for o in (1, 3, 2):
        sends[o, 4].wait_recv()
    row_t = [row[k, V:, :] for k in range(4)]
    row_t10 = mm(row_t[0], row_t[1])
    row_t32 = mm(row_t[2], row_t[3])
    row_10[V:, :] = row_t10
    row_all[...] = mm(row_t10, row_t32)
    gives = {}
    for o in (2, 1, 3):
        gives[o] = copy(
            row_all, y_buf.at[y, pl.ds(Q, K)], ya_sem, o, {"seq_0": turn(y, o)}
        )
        gives[o].start()
        started.append(gives[o])
    y_buf[y, Q:, :] = row_all[...]
    weights_1 = weights(row_t[1])
    weights_3 = weights(row_t[3])
    weights_32 = weights(row_t32)
    for part in (2, 1, 3, 0):
        rows = quarter(part)
        for o in (1, 3, 2):
            sends[o, part].wait_recv()
        part_10 = fold(dot(side(row[0, rows, :]), weights_1)) + row[1, rows, :]
        part_32 = fold(dot(side(row[2, rows, :]), weights_3)) + row[3, rows, :]
        row_10[rows, :] = part_10
        total = fold(dot(side(part_10), weights_32)) + part_32
        if part == 0:
            y_buf[y, :Q, :] = total
        else:
            y_send[part] = total
            gives[4 + part] = copy(
                y_send.at[part],
                y_buf.at[y, pl.ds(0, Q)],
                ya_sem,
                4 + part,
                {"seq_0": turn(y, part)},
            )
            gives[4 + part].start()
            started.append(gives[4 + part])
    for o in (1, 3, 2):
        gives[o].wait_recv()
    plane_t = [y_buf[k, Q:, :] for k in range(4)]
    plane_t10 = mm(plane_t[0], plane_t[1])
    plane_t32 = mm(plane_t[2], plane_t[3])
    trans = mm(plane_t10, plane_t32)

    even = lax.rem(z, 2) == 0
    next_one = {"grp": lax.rem(z + 1, planes)}
    size = Q // PIECES
    pieces = [pl.ds(i * size, size) for i in range(PIECES)]
    two_on = {"grp": lax.rem(z + 2, planes)}
    give_trans = copy(
        p_send.at[pl.ds(Q, K)], p_buf.at[pl.ds(Q, K)], p_sem, PIECES, next_one
    )
    give_state, jump, step = [], [], []
    for i, rows in enumerate(pieces):
        give_state.append(copy(p_send.at[rows], p_buf.at[rows], p_sem, i, next_one))
        jump.append(copy(z_out.at[rows], z_in.at[rows], z_sem, i, two_on))
        step.append(copy(z_out.at[rows], z_in.at[rows], z_sem, PIECES + i, next_one))
    far = {}
    for o in (3, 4):
        there = {"grp": lax.rem(z + o, planes)}
        far[o] = [
            copy(z_out.at[rows], z_in.at[rows], z_sem, (o - 1) * PIECES + i, there)
            for i, rows in enumerate(pieces)
        ]
    hand = {1: copy(h_send, h_buf, h_sem, 0, next_one)}
    hand[2] = copy(h_send, h_buf, h_sem, 1, two_on)

    @pl.when(even & (z > 0))
    def _():
        p_send[Q:, :] = trans
        give_trans.start()

    for o in (3, 1, 2):
        gives[4 + o].wait_recv()
    plane_s = [y_buf[k, :Q, :] for k in range(4)]
    plane_s10 = mm(plane_s[0], plane_t[1]) + plane_s[1]
    plane_s32 = mm(plane_s[2], plane_t[3]) + plane_s[3]
    total = mm(plane_s10, plane_t32) + plane_s32

    @pl.when(even)
    def _():
        p_send[:Q, :] = total
        for part in give_state:
            part.start()

    row_210[...] = joined(row_10[...], row[2])
    plane_10 = jnp.concatenate([plane_s10, plane_t10], axis=0)
    plane_210 = joined(plane_10, y_buf[2])
    down_y = [side(plane_t[0]), side(plane_t10), side(plane_210[Q:])]
    down_x = [side(row_t[0]), side(row_t10), side(row_210[V:, :])]

    @pl.when(z == 0)
    def _():
        enter[...] = jnp.zeros_like(enter)

    @pl.when(z == 1)
    def _():
        for i, rows in enumerate(pieces):
            give_state[i].wait_recv()
            z_out[rows, :] = mm(p_buf[rows, :], trans) + total[i * size : (i + 1) * size]
            jump[i].start()
        for part in step:
            part.start()
        enter[...] = p_buf[:Q, :]

    @pl.when(z == 3)
    def _():
        give_trans.wait_recv()
        two_t = mm(p_buf[Q:, :], trans)
        for part in give_state:
            part.wait_recv()
        two_s = mm(p_buf[:Q, :], trans) + total
        for i, rows in enumerate(pieces):
            jump[i].wait_recv()
            z_out[rows, :] = mm(z_in[rows, :], two_t) + two_s[i * size : (i + 1) * size]
            far[4][i].start()
        for part in far[3] + jump + step:
            part.start()
        enter[...] = entered(z_in[...], p_buf[...])

    @pl.when(z == 5)
    def _():
        give_trans.wait_recv()
        h_send[Q:, :] = mm(p_buf[Q:, :], trans)
        for part in give_state:
            part.wait_recv()
        h_send[:Q, :] = mm(p_buf[:Q, :], trans) + total
        hand[2].start()
        hand[1].start()
        for part in jump:
            part.wait_recv()
        enter[...] = entered(z_in[...], p_buf[...])

    @pl.when(z == 6)
    def _():
        hand[1].wait_recv()
        for part in far[3]:
            part.wait_recv()
        enter[...] = entered(z_in[...], h_buf[...])

    @pl.when(z == 7)
    def _():
        give_trans.wait_recv()
        for part in give_state:
            part.wait_recv()
        hand[2].wait_recv()
        three = joined(h_buf[...], p_buf[...])
        for part in far[4]:
            part.wait_recv()
        enter[...] = entered(z_in[...], three)

    @pl.when((z == 2) | (z == 4))
    def _():
        for part in step:
            part.wait_recv()
        enter[...] = z_in[...]

    state = enter[...]
    r_send[0] = state
    r_send[1] = through(state, down_y[0]) + plane_s[0]
    r_send[2] = through(state, down_y[1]) + plane_s10
    r_send[3] = through(state, down_y[2]) + plane_210[:Q]
    mine = pl.ds(pl.multiple_of(y * Q, Q), Q)
    sends = {}
    for o in (2, 1, 3):
        to = turn(y, o)
        sends[o] = copy(r_send.at[to], r_buf.at[mine], yb_sem, o, {"seq_0": to})
        sends[o].start()
        started.append(sends[o])
    r_buf[mine, :] = r_send[y]
    arrivals = {1: [], 2: [], 3: []}
    for o in (0, 1, 3, 2):
        if o > 0:
            sends[o].wait_recv()
        part = pl.ds(pl.multiple_of(turn(y, -o) * Q, Q), Q)
        state = r_buf[part, :]
        x_send[0, part, :] = state
        x_send[1, part, :] = through(state, down_x[0]) + row[0, part, :]
        x_send[2, part, :] = through(state, down_x[1]) + row_10[part, :]
        x_send[3, part, :] = through(state, down_x[2]) + row_210[part, :]
        for a in (2, 1, 3):
            to = turn(x, a)
            sent = copy(
                x_send.at[to, part], x_buf.at[x, part], xb_sem, 4 * a + o, {"seq_1": to}
            )
            sent.start()
            started.append(sent)
            arrivals[a].append(sent)
        x_buf[x, part, :] = x_send[x, part, :]

    def read_out(head):
        both = own[head] + mm_nt(eff[head], full[head])
        vf0[pl.ds(head, T, stride=H), :] = both[:, :K]
        vf1[pl.ds(head, T, stride=H), :] = both[:, K:]

    swaps = []
    for a in (0, 1, 3, 2):
        j = turn(x, -a)
        if a > 0:
            for sent in arrivals[a]:
                sent.wait_recv()
        first = x_buf[j]
        second = entered(first, pair[0, j])
        head = HH * c + j
        full[head] = jnp.where(c == 0, first, second)
        c_send[a] = jnp.where(c == 0, second, first)
        swap = copy(c_send.at[a], full.at[head], back_sem, a, {"seq_2": 1 - c})
        swap.start()
        started.append(swap)
        swaps.append((swap, j))
        read_out(head)
    for swap, j in swaps:
        swap.wait_recv()
        read_out(HH * (1 - c) + j)
    o_ref[:, :, :K] = vf0[...].reshape(T, H, K).astype(BF16)
    o_ref[:, :, K:] = vf1[...].reshape(T, H, K).astype(BF16)

    for sent in started:
        sent.wait_send()

    @pl.when(even)
    def _():
        for part in give_state:
            part.wait_send()

    @pl.when(even & (z > 0))
    def _():
        give_trans.wait_send()

    @pl.when((z == 1) | (z == 3))
    def _():
        for part in jump + step:
            part.wait_send()

    @pl.when(z == 3)
    def _():
        for part in far[3] + far[4]:
            part.wait_send()

    @pl.when(z == 5)
    def _():
        hand[1].wait_send()
        hand[2].wait_send()


def body(*given):
    queries, key_rows, value_rows, log_gate, beta_rate = [pltpu.with_memory_space_constraint(a, pltpu.HBM) for a in given]
    dma = pltpu.SemaphoreType.DMA

    def room(*shape):
        return pltpu.VMEM(shape, F32)

    return pl.pallas_call(
        scan_kernel,
        out_shape=jax.ShapeDtypeStruct((T, H, V), BF16),
        in_specs=[pl.BlockSpec(memory_space=pltpu.HBM)] * 5,
        out_specs=pl.BlockSpec(memory_space=pltpu.VMEM),
        scratch_shapes=[
            pltpu.VMEM((T, H, K), BF16),
            pltpu.VMEM((T, H, K), BF16),
            pltpu.VMEM((T, H, V), BF16),
            room(H, T),
            room(H, T),
            room(T * H, K),
            room(T * H, K),
            room(T * H, K),
            room(T * H, K),
            room(H, K, T),
            room(H, V, T),
            room(H, T, K),
            room(H, T, V),
            room(H, ROWS, K),
            room(2, HH, ROWS, K),
            room(4, ROWS, K),
            room(4, ROWS, K),
            room(ROWS, K),
            room(ROWS, K),
            room(K, K),
            room(4, Q, K),
            room(4, Q + K, K),
            room(Q + K, K),
            room(Q + K, K),
            room(Q + K, K),
            room(Q + K, K),
            room(Q, K),
            room(Q, K),
            room(Q, K),
            room(4, Q, K),
            room(V, K),
            room(4, V, K),
            room(4, V, K),
            room(4, V, K),
            room(H, V, K),
            dma((5,)),
            dma((2, 8)),
            dma((2, 15)),
            dma((2, 8)),
            dma((2, PIECES + 1)),
            dma((2, 2)),
            dma((2, 4 * PIECES)),
            dma((2, 4)),
            dma((2, 16)),
            dma((2, 4)),
        ],
        compiler_params=pltpu.CompilerParams(
            collective_id=0, has_side_effects=True, vmem_limit_bytes=48 * 1024 * 1024
        ),
        name="scan",
    )(queries, key_rows, value_rows, log_gate, beta_rate)


def solution(mesh):
    finer = Mesh(
        mesh.devices.reshape(4, 4, 2, mesh.shape["grp"]), ("seq_0", "seq_1", "seq_2", "grp")
    )
    placed = (
        P(GRP_SEQ, None, None),
        P(GRP_SEQ, None, None),
        P(GRP_SEQ, None, None),
        P(None, GRP_SEQ),
        P(None, GRP_SEQ),
    )
    return jax.shard_map(
        body, mesh=finer, in_specs=placed, out_specs=P(GRP_SEQ, None, None), check_vma=False
    )
```
